32 devices in a mesh: grp: 16 (over z, x, core), mode: 2 (over y).
Axes of the slice: x: 2, y: 2, z: 4, core: 2. Of those that a mesh axis runs over, the one named last changes fastest.
Arguments:
- probe: float32 [2, 8, 512, 512], P(None, 'mode'), may hold values from -3 to 3
- prev_direction: float32 [2, 8, 512, 512], P(None, 'mode'), may hold values from -0.6 to 0.6
- prev_norm: float32 [8], P('mode'), may hold values from 0.5 to 4
- object_tile: bfloat16 [2, 10240, 640], P(None, 'grp'), may hold values from -4 to 4
- offsets: int32 [32, 2], P('grp'), may hold values from 0 to 128
- amplitude: bfloat16 [32, 512, 512], P('grp'), may hold values from 0.5 to 3.5
Outputs:
- new_probe: float32 [2, 8, 512, 512], P(None, 'mode')
- new_direction: float32 [2, 8, 512, 512], P(None, 'mode')
- new_norm: float32 [8], P('mode')
The draws below stay inside these ranges and needn't reach their ends.
All inputs are finite; a program needn't handle non-finite values.
Results may differ from the reference program's by a relative error of at most 0.0045.
Values sent between devices are 32-bit elements; how exact they have to be, the bound alone decides.
A program may use at most 128 MiB of HBM per device.

```python
import math
import jax
import jax.numpy as jnp
from jax import lax

M = 8
N = 512
POS_DEV = 2
SPAN = 128
OBJ = 640
POSITIONS = 32
N_GRP = 16


def draw_object_tile(key, part):
    phase_key = jax.random.fold_in(key, 11)
    value_key = jax.random.fold_in(key, 12)
    phases = jax.random.uniform(phase_key, (N_GRP,), jnp.float32, 0.0, 2.0 * math.pi)
    rows = jnp.arange(N_GRP * OBJ, dtype=jnp.int32)
    local = (rows % OBJ).astype(jnp.float32)
    group = rows // OBJ
    shift = jnp.sum(jnp.where(group[:, None] == jnp.arange(N_GRP, dtype=jnp.int32)[None, :], phases[None, :], 0.0), axis=1)
    envelope = jnp.exp(0.9 * jnp.sin(2.0 * math.pi * local / OBJ + shift))
    values = 0.7 * jax.random.normal(value_key, (2, N_GRP * OBJ, OBJ), jnp.float32)
    values = jnp.clip(values * envelope[None, :, None], -4.0, 4.0)
    return values.astype(jnp.bfloat16)


def plant(values, rng, smallest, top_value):
    index_at = [jax.random.randint(jax.random.fold_in(rng, axis), (), 0, length) for axis, length in enumerate(values.shape)]
    longest = values.shape.index(max(values.shape))
    beside = index_at[:longest] + [(index_at[longest] + 1) % values.shape[longest]] + index_at[longest + 1:]
    return values.at[tuple(index_at)].set(smallest).at[tuple(beside)].set(top_value)


def shard_levels(stream_key, dims, cuts, smallest, largest):
    def one(dim, parts):
        steps = jax.random.uniform(jax.random.fold_in(jax.random.fold_in(stream_key, 6), dim), (parts,), jnp.float32, smallest / len(cuts), largest / len(cuts))
        return jnp.repeat(jnp.exp(steps), dims[dim] // parts).reshape((-1,) + (1,) * (len(dims) - dim - 1))

    gain = one(*cuts[0])
    for cut in cuts[1:]:
        gain = gain * one(*cut)
    return gain


def gaussian(stream_key, shape, spread, reach, shards=(), held_as=jnp.bfloat16):
    drawn = jax.random.normal(stream_key, shape, jnp.float32) * spread
    if len(shards) > 0:
        drawn = shard_levels(stream_key, shape, shards, -0.22, 0.18) * drawn
    return jnp.clip(drawn, min=-reach, max=reach).astype(held_as)


def setup_inputs(seed: int = 0) -> dict:
    keys = jax.random.split(jax.random.key(seed), 7)
    probe = gaussian(keys[0], (2, M, N, N), 0.5, 3.0, ((1, 2),), jnp.float32)
    prev_direction = gaussian(keys[1], (2, M, N, N), 0.1, 0.6, ((1, 2),), jnp.float32)
    prev_norm = jnp.clip(jnp.exp(math.log(4.0) - 2.0794415 * jax.random.uniform(keys[2], (M,), jnp.float32) ** shard_levels(keys[2], (M,), ((0, 2),), -0.2, 0.2)), 0.5, 4.0)
    object_tile = draw_object_tile(jax.random.fold_in(keys[6], 71), 0)
    offsets = plant(jax.random.randint(keys[4], (POSITIONS, 2), 0, SPAN + 1), jax.random.fold_in(keys[4], 1), 0, SPAN).astype(jnp.int32)
    amplitude = jnp.clip(0.5 + 3.0 * jax.random.uniform(keys[5], (POSITIONS, N, N), jnp.float32) ** shard_levels(keys[5], (POSITIONS, N, N), ((0, 16),), -0.2, 0.2), 0.5, 3.5).astype(jnp.bfloat16)
    return {"probe": probe, "prev_direction": prev_direction, "prev_norm": prev_norm, "object_tile": object_tile, "offsets": offsets, "amplitude": amplitude}


def tables(width, sign):
    index = jnp.arange(width, dtype=jnp.int32)
    product = index[:, None] * index[None, :] % width
    angle = -2.0 * math.pi / width * product.astype(jnp.float32)
    scale = 1.0 / math.sqrt(width)
    real_part = (jnp.cos(angle) * scale).astype(jnp.bfloat16)
    imag_part = (sign * jnp.sin(angle) * scale).astype(jnp.bfloat16)
    right = jnp.concatenate([jnp.concatenate([real_part, imag_part], 1), jnp.concatenate([-imag_part, real_part], 1)], 0)
    left = jnp.concatenate([jnp.concatenate([real_part, -imag_part], 1), jnp.concatenate([imag_part, real_part], 1)], 0)
    return (right, left)

def transform(real_in, imag_in, right, left):
    count, width = (real_in.shape[0], real_in.shape[1])
    joined = jnp.concatenate([real_in, imag_in], axis=2).reshape(count * width, 2 * width)
    half = jnp.dot(joined.astype(jnp.float32), right.astype(jnp.float32), preferred_element_type=jnp.float32)
    half = half.astype(jnp.bfloat16).reshape(count, width, 2 * width)
    stacked = jnp.concatenate([half[:, :, :width], half[:, :, width:]], axis=1)
    out = jnp.einsum('ab,mbc->mac', left.astype(jnp.float32), stacked.astype(jnp.float32))
    return (out[:, :width], out[:, width:])

def reference(probe, prev_direction, prev_norm, object_tile, offsets, amplitude):
    fwd_right, fwd_left = tables(N, 1.0)
    inv_right, inv_left = tables(N, -1.0)
    probe_re, probe_im = (probe[0], probe[1])

    def visit(carry, index):
        grad_re, grad_im, illum = carry
        group = index // POS_DEV
        row = (group * OBJ + offsets[index, 0]).astype(jnp.int32)
        col = offsets[index, 1].astype(jnp.int32)
        patch = lax.dynamic_slice(object_tile, (jnp.int32(0), row, col), (2, N, N)).astype(jnp.float32)
        obj_re, obj_im = (patch[0], patch[1])
        exit_re = (probe_re * obj_re - probe_im * obj_im).astype(jnp.bfloat16)
        exit_im = (probe_re * obj_im + probe_im * obj_re).astype(jnp.bfloat16)
        wave_re, wave_im = transform(exit_re, exit_im, fwd_right, fwd_left)
        intensity = lax.optimization_barrier(jnp.sum(wave_re * wave_re + wave_im * wave_im, axis=0))
        ratio = amplitude[index].astype(jnp.float32) / jnp.sqrt(intensity + 1.0)
        fixed_re = (ratio * wave_re).astype(jnp.bfloat16)
        fixed_im = (ratio * wave_im).astype(jnp.bfloat16)
        back_re, back_im = transform(fixed_re, fixed_im, inv_right, inv_left)
        diff_re = back_re - exit_re.astype(jnp.float32)
        diff_im = back_im - exit_im.astype(jnp.float32)
        grad_re = grad_re + obj_re * diff_re + obj_im * diff_im
        grad_im = grad_im + obj_re * diff_im - obj_im * diff_re
        illum = illum + obj_re * obj_re + obj_im * obj_im
        return ((grad_re, grad_im, illum), None)
    start = (jnp.zeros((M, N, N), jnp.float32), jnp.zeros((M, N, N), jnp.float32), jnp.zeros((N, N), jnp.float32))
    (grad_re, grad_im, illum), unused = lax.scan(visit, start, jnp.arange(POSITIONS, dtype=jnp.int32))
    total = jnp.sum(illum)
    denom = illum + total / (N * N)
    pre_re = grad_re / denom
    pre_im = grad_im / denom
    new_norm = lax.optimization_barrier(jnp.mean(grad_re * pre_re + grad_im * pre_im, axis=(1, 2)))
    beta = (new_norm / prev_norm)[:, None, None]
    dir_re = pre_re + beta * prev_direction[0]
    dir_im = pre_im + beta * prev_direction[1]
    upper = lax.optimization_barrier(jnp.mean(grad_re * dir_re + grad_im * dir_im, axis=(1, 2)))
    lower = lax.optimization_barrier(jnp.mean(illum * (dir_re * dir_re + dir_im * dir_im), axis=(1, 2)))
    alpha = (upper / (lower + 1.0))[:, None, None]
    new_direction = jnp.stack([dir_re, dir_im])
    new_probe = jnp.stack([probe_re + alpha * dir_re, probe_im + alpha * dir_im])
    return (new_probe, new_direction, new_norm)
```

```python
import functools
import math

import jax
import jax.numpy as jnp
from jax import lax
from jax.experimental import pallas as pl
from jax.experimental.pallas import tpu as pltpu
from jax.sharding import PartitionSpec as P

MESH = pl.DeviceIdType.MESH
VMEM_LIMIT = 60 * 1024 * 1024
TILE = 256


def base_table(width):
    index = jnp.arange(width, dtype=jnp.int32)
    product = index[:, None] * index[None, :] % width
    angle = -2.0 * math.pi / width * product.astype(jnp.float32)
    scale = 1.0 / math.sqrt(width)
    real_part = (jnp.cos(angle) * scale).astype(jnp.bfloat16)
    imag_part = (jnp.sin(angle) * scale).astype(jnp.bfloat16)
    return jnp.stack([real_part, imag_part])


def build_pair(base_ref, plus, minus):
    width = base_ref.shape[1]
    cosine, sine = base_ref[0], base_ref[1]
    for ref, sign in ((plus, 1), (minus, -1)):
        ref[:width, :width] = cosine
        ref[width:, width:] = cosine
        ref[:width, width:] = sine if sign > 0 else -sine
        ref[width:, :width] = -sine if sign > 0 else sine


def transform(joined, stacked, right, left, emit):
    width = joined.shape[0]
    tile = min(TILE, width)

    def first(step, carry):
        at = pl.multiple_of(step * tile, tile)
        half = jnp.dot(joined[pl.ds(at, tile), :], right[...], preferred_element_type=jnp.float32)
        half = half.astype(jnp.bfloat16)
        stacked[pl.ds(at, tile), :] = half[:, :width]
        stacked[pl.ds(at + width, tile), :] = half[:, width:]
        return carry

    def second(step, carry):
        at = pl.multiple_of(step * tile, tile)
        rows = pl.ds(at, tile)
        real = jnp.dot(left[rows, :], stacked[...], preferred_element_type=jnp.float32)
        imag = jnp.dot(left[pl.ds(at + width, tile), :], stacked[...], preferred_element_type=jnp.float32)
        emit(rows, real, imag)
        return carry

    lax.fori_loop(0, width // tile, first, 0)
    lax.fori_loop(0, width // tile, second, 0)


def forward_kernel(base_ref, probe_ref, patch_ref, wave_ref, exit_ref, sum_ref, plus, minus, joined, stacked):
    mode = pl.program_id(0)
    width = sum_ref.shape[0]
    tile = 64

    @pl.when(mode == 0)
    def _():
        build_pair(base_ref, plus, minus)
        sum_ref[...] = jnp.zeros_like(sum_ref)

    def leave(step, carry):
        rows = pl.ds(pl.multiple_of(step * tile, tile), tile)
        obj_re = patch_ref[0, rows, :].astype(jnp.float32)
        obj_im = patch_ref[1, rows, :].astype(jnp.float32)
        pro_re, pro_im = probe_ref[0, 0, rows, :], probe_ref[1, 0, rows, :]
        exit_re = (pro_re * obj_re - pro_im * obj_im).astype(jnp.bfloat16)
        exit_im = (pro_re * obj_im + pro_im * obj_re).astype(jnp.bfloat16)
        joined[rows, :width] = exit_re
        joined[rows, width:] = exit_im
        exit_ref[0, 0, rows, :] = exit_re
        exit_ref[0, 1, rows, :] = exit_im
        return carry

    lax.fori_loop(0, width // tile, leave, 0)

    def emit(rows, real, imag):
        wave_ref[0, 0, rows, :] = real
        wave_ref[0, 1, rows, :] = imag
        sum_ref[rows, :] += real * real + imag * imag

    transform(joined, stacked, plus, minus, emit)


def backward_kernel(first, base_ref, total_ref, amp_ref, wave_ref, exit_ref, patch_ref, *rest):
    if first:
        grad_in, (grad_ref, plus, minus, joined, stacked, ratio) = None, rest
    else:
        grad_in, grad_ref, plus, minus, joined, stacked, ratio = rest
    width = total_ref.shape[0]
    tile = 64

    @pl.when(pl.program_id(0) == 0)
    def _():
        build_pair(base_ref, plus, minus)

        def scale(step, carry):
            rows = pl.ds(pl.multiple_of(step * tile, tile), tile)
            ratio[rows, :] = amp_ref[0, rows, :].astype(jnp.float32) / jnp.sqrt(total_ref[rows, :] + 1.0)
            return carry

        lax.fori_loop(0, width // tile, scale, 0)

    def fix(step, carry):
        rows = pl.ds(pl.multiple_of(step * tile, tile), tile)
        joined[rows, :width] = (ratio[rows, :] * wave_ref[0, 0, rows, :]).astype(jnp.bfloat16)
        joined[rows, width:] = (ratio[rows, :] * wave_ref[0, 1, rows, :]).astype(jnp.bfloat16)
        return carry

    lax.fori_loop(0, width // tile, fix, 0)

    def emit(rows, real, imag):
        obj_re = patch_ref[0, rows, :].astype(jnp.float32)
        obj_im = patch_ref[1, rows, :].astype(jnp.float32)
        diff_re = real - exit_ref[0, 0, rows, :].astype(jnp.float32)
        diff_im = imag - exit_ref[0, 1, rows, :].astype(jnp.float32)
        add_re = obj_re * diff_re + obj_im * diff_im
        add_im = obj_re * diff_im - obj_im * diff_re
        if grad_in is not None:
            add_re = grad_in[0, 0, rows, :] + add_re
            add_im = grad_in[0, 1, rows, :] + add_im
        grad_ref[0, 0, rows, :] = add_re
        grad_ref[0, 1, rows, :] = add_im

    transform(joined, stacked, minus, plus, emit)


def fold_lanes(block):
    rows, width = block.shape
    lanes = min(128, width)
    acc = jnp.sum(block.reshape(rows // 8, 8, width), axis=0)
    out = acc[:, :lanes]
    for at in range(lanes, width, lanes):
        out = out + acc[:, at : at + lanes]
    return out


class Spot:
    def __init__(self, outer, inner, cores):
        me = lax.axis_index("grp")
        self.me = me
        self.sizes = (outer, inner, cores)
        self.count = outer * inner * cores
        self.core = lax.rem(me, cores)
        self.inner = lax.rem(me // cores, inner)
        self.outer = me // (cores * inner)
        self.stride = {"core": 1, "inner": cores, "outer": cores * inner}

    def at(self, line, step):
        return {"grp": self.me + step * self.stride[line]}

    def partner(self):
        return {"grp": self.me + 1 - 2 * self.core}


def remote(src, dst, send, recv, device):
    return pltpu.make_async_remote_copy(
        src_ref=src, dst_ref=dst, send_sem=send, recv_sem=recv, device_id=device, device_id_type=MESH
    )


class Line:
    def __init__(self, spot, name, length, place):
        self.spot, self.name, self.length, self.place = spot, name, length, place

    def scatter(self, chunk, slots, send, recv):
        size, u = self.length, self.place

        def take(slot, into):
            got = remote(slots.at[slot], slots.at[slot], send.at[0], recv.at[slot], self.spot.at(self.name, 0))
            got.wait_recv()
            into[...] += slots[slot]

        def push(k, step, slot):
            remote(chunk(k), slots.at[slot], send.at[k], recv.at[slot], self.spot.at(self.name, step)).start()

        for step in range(size - 1):
            right, left = size - 1 - step, step

            @pl.when(u < right)
            def _():
                @pl.when(u > 0)
                def _():
                    take(right + 1, chunk(right))

                push(right, 1, right + 1)

            @pl.when(u > left)
            def _():
                @pl.when(u < size - 1)
                def _():
                    take(left, chunk(left))

                push(left, -1, left)

            yield

        @pl.when(u > 0)
        def _():
            take(u + 1, chunk(u))

        @pl.when(u < size - 1)
        def _():
            take(u, chunk(u))

    def scatter_end(self, chunk, slots, send, recv):
        for k in range(self.length):
            @pl.when(self.place != k)
            def _():
                remote(chunk(k), slots.at[0], send.at[k], recv.at[0], self.spot.at(self.name, 0)).wait_send()

    def gather(self, chunk, send, recv):
        size, u = self.length, self.place

        def push(k, way, step):
            remote(chunk(k), chunk(k), send.at[way, k], recv.at[k], self.spot.at(self.name, step)).start()

        def take(k):
            remote(chunk(k), chunk(k), send.at[0, 0], recv.at[k], self.spot.at(self.name, 0)).wait_recv()

        for step in range(size):
            low, high = u - step, u + step

            @pl.when(low >= 0)
            def _():
                if step > 0:
                    take(low)

                @pl.when(u < size - 1)
                def _():
                    push(low, 0, 1)

            @pl.when(high < size)
            def _():
                if step > 0:
                    take(high)

                @pl.when(u > 0)
                def _():
                    push(high, 1, -1)

            if step < size - 1:
                yield

    def gather_end(self, chunk, send, recv):
        size, u = self.length, self.place
        for k in range(size):
            for way in range(2):
                @pl.when((u < size - 1) & (u >= k) if way == 0 else (u > 0) & (u <= k))
                def _():
                    remote(chunk(k), chunk(k), send.at[way, k], recv.at[k], self.spot.at(self.name, 0)).wait_send()


def whole(shape):
    return pl.BlockSpec(shape, lambda *_: (0,) * len(shape))


def table_scratch(width):
    return [
        pltpu.VMEM((2 * width, 2 * width), jnp.bfloat16),
        pltpu.VMEM((2 * width, 2 * width), jnp.bfloat16),
        pltpu.VMEM((width, 2 * width), jnp.bfloat16),
        pltpu.VMEM((2 * width, width), jnp.bfloat16),
    ]


def params():
    return pltpu.CompilerParams(dimension_semantics=("arbitrary",), vmem_limit_bytes=VMEM_LIMIT)


def cost(modes, width, moved):
    return pl.CostEstimate(flops=modes * 16 * width**3, bytes_accessed=moved, transcendentals=0)


def forward(base, probe, patch):
    modes, width = probe.shape[1], probe.shape[2]
    return pl.pallas_call(
        forward_kernel,
        grid=(modes,),
        in_specs=[
            whole(base.shape),
            pl.BlockSpec((2, 1, width, width), lambda m: (0, m, 0, 0)),
            whole(patch.shape),
        ],
        out_specs=[
            pl.BlockSpec((1, 2, width, width), lambda m: (m, 0, 0, 0)),
            pl.BlockSpec((1, 2, width, width), lambda m: (m, 0, 0, 0)),
            whole((width, width)),
        ],
        out_shape=[
            jax.ShapeDtypeStruct((modes, 2, width, width), jnp.float32),
            jax.ShapeDtypeStruct((modes, 2, width, width), jnp.bfloat16),
            jax.ShapeDtypeStruct((width, width), jnp.float32),
        ],
        scratch_shapes=table_scratch(width),
        compiler_params=params(),
        cost_estimate=cost(modes, width, modes * width * width * 20),
        name="forward",
    )(base, probe, patch)


def backward(base, total, amplitude, index, wave, exits, patch, grad, start, count):
    width = total.shape[0]
    at = lambda m: (m + start, 0, 0, 0)
    block = (1, 2, width, width)
    operands = [base, total, amplitude, wave, exits, patch]
    in_specs = [
        whole(base.shape),
        whole(total.shape),
        pl.BlockSpec((1, width, width), lambda m: (index, 0, 0)),
        pl.BlockSpec(block, at),
        pl.BlockSpec(block, at),
        whole(patch.shape),
    ]
    if grad is not None:
        operands.append(grad)
        in_specs.append(pl.BlockSpec(block, at))
    return pl.pallas_call(
        functools.partial(backward_kernel, grad is None),
        grid=(count,),
        in_specs=in_specs,
        out_specs=pl.BlockSpec(block, lambda m: (m, 0, 0, 0)),
        out_shape=jax.ShapeDtypeStruct((count, 2, width, width), jnp.float32),
        scratch_shapes=table_scratch(width) + [pltpu.VMEM((width, width), jnp.float32)],
        compiler_params=params(),
        cost_estimate=cost(count, width, count * width * width * 24),
        name="backward",
    )(*operands)


def split_lines(cores_total):
    cores = 2 if cores_total % 2 == 0 else 1
    chips = cores_total // cores
    inner = 1
    while inner * inner * 2 <= chips and chips % (inner * 2) == 0:
        inner *= 2
    inner = inner if inner * inner <= chips else inner // 2
    return chips // inner, inner, cores


class Shares:
    def __init__(self, spot, width):
        outer, inner, cores = spot.sizes
        self.part = width // cores
        self.half = self.part // 2
        self.own = self.half // (outer * inner)
        self.base = (spot.core * self.part, spot.core * self.part + self.half)
        a_big, b_big = self.half // inner, self.half // outer
        self.big = (a_big, b_big)
        self.first = ("inner", "outer")
        place = {"inner": spot.inner, "outer": spot.outer}
        size = {"inner": inner, "outer": outer}
        self.lines = tuple(Line(spot, name, size[name], place[name]) for name in ("inner", "outer"))
        self.offset = (
            spot.inner * a_big + spot.outer * self.own,
            spot.outer * b_big + spot.inner * self.own,
        )
        self.group = (spot.inner * a_big, spot.outer * b_big)

    def order(self, path):
        return (self.lines[0], self.lines[1]) if path == 0 else (self.lines[1], self.lines[0])


def rows_at(ref, start, count):
    return ref.at[:, pl.ds(pl.multiple_of(start, 8), count), :]


def reduce_kernel(
    shape, modes, width, grad_ref, illum_ref, dir_ref, pre_ref, sums_ref,
    held, held_i, prev, shift_in, shift_all, sums_in, sums_all, *rest,
):
    outer, inner, cores = shape
    spot = Spot(outer, inner, cores)
    share = Shares(spot, width)
    (slots, islots, core_s, core_r, sc_s, sc_r, ga_s, ga_r, isc_s, isc_r, back_s, back_r, dir_sem, bc_s, bc_r) = (
        rest[0:4], rest[4:8], *rest[8:10], rest[10:14], rest[14:18], rest[18:22], rest[22:26],
        rest[26:30], rest[30:34], *rest[34:],
    )
    me, count = spot.me, spot.count
    pixels = float(width * width)

    barrier = pltpu.get_barrier_semaphore()
    for step in range(1, count):
        pl.semaphore_signal(barrier, inc=1, device_id={"grp": lax.rem(me + step, count)}, device_id_type=MESH)

    loads = []
    for path in range(2):
        start = pl.multiple_of(share.base[path] + share.offset[path], 8)
        for m in range(modes):
            load = pltpu.make_async_copy(
                dir_ref.at[:, m, pl.ds(start, share.own), :], prev.at[path, m], dir_sem.at[path, m]
            )
            load.start()
            loads.append(load)
    pl.semaphore_wait(barrier, count - 1)

    def core_send(src, dst, item):
        return remote(src, dst, core_s.at[item], core_r.at[item], spot.partner())

    def partial(m):
        return grad_ref.at[m] if m < modes else illum_ref

    def keep(m):
        return held.at[m] if m < modes else held_i

    def give(m):
        other = (1 - spot.core) * share.part
        return core_send(rows_at(partial(m), other, share.part), keep(m), m)

    items = [modes] + list(range(modes))
    for m in items:
        give(m).start()

    def pair(m, path):
        if m < modes:
            one, two = 2 * path, 2 * path + 1
            return [(slots[k].at[m], sc_s[k].at[m], sc_r[k].at[m]) for k in (one, two)]
        return [(islots[k], isc_s[k], isc_r[k]) for k in (2 * path, 2 * path + 1)]

    def scatter_parts(m, path):
        first, second = share.order(path)
        at = path * share.half
        top = lambda k: rows_at(keep(m), at + k * share.big[path], share.big[path])
        low = lambda k: rows_at(keep(m), at + share.group[path] + k * share.own, share.own)
        return [(line, chunk) + sems for line, chunk, sems in zip((first, second), (top, low), pair(m, path))]

    def gather_parts(m, path):
        second, first = share.order(path)
        base = share.base[path]
        low = lambda k: rows_at(pre_ref.at[m], base + share.group[path] + k * share.own, share.own)
        top = lambda k: rows_at(pre_ref.at[m], base + k * share.big[path], share.big[path])
        sems = [(ga_s[k].at[m], ga_r[k].at[m]) for k in (2 * path, 2 * path + 1)]
        return [(line, chunk) + pairs for line, chunk, pairs in zip((first, second), (low, top), sems)]

    def home(m, path):
        block = rows_at(pre_ref.at[m], share.base[path], share.half)
        return remote(block, block, back_s.at[m, path], back_r.at[m, path], spot.partner())

    def broadcast(src, dst, which):
        copies = []
        for step in range(1, count):
            to = lax.rem(me + step, count)
            copies.append(remote(src, dst.at[step], bc_s.at[which, step], bc_r.at[which, step], {"grp": to}))
        return copies

    def own_illum(path):
        at = pl.multiple_of(path * share.half + share.offset[path], 8)
        return held_i[0, pl.ds(at, share.own), :]

    def scatter(m, path):
        if path == 0:
            give(m).wait_recv()
            held_m, mine = keep(m), partial(m)
            step = 32 if share.part % 32 == 0 else share.part

            def add(i, carry):
                rows = pl.ds(pl.multiple_of(i * step, 8), step)
                held_m[:, rows, :] += mine[:, pl.ds(pl.multiple_of(spot.core * share.part + i * step, 8), step), :]
                return carry

            lax.fori_loop(0, share.part // step, add, 0)
        for line, chunk, slot, send, recv in scatter_parts(m, path):
            yield from line.scatter(chunk, slot, send, recv)

    def illum_done():
        tile = fold_lanes(own_illum(0)) + fold_lanes(own_illum(1))
        shift_in[...] = tile
        for copy in broadcast(shift_in, shift_all, 0):
            copy.start()
        shift_all[0] = tile

    def shift_value():
        for copy in broadcast(shift_in, shift_all, 0):
            copy.wait_recv()
        return jnp.sum(shift_all[...]) / pixels

    def mode(m, path, shift):
        yield from scatter(m, path)
        at = pl.multiple_of(path * share.half + share.offset[path], 8)
        rows = pl.ds(at, share.own)
        to = pl.ds(pl.multiple_of(share.base[path] + share.offset[path], 8), share.own)
        light = own_illum(path)
        loads[path * modes + m].wait()
        g_re, g_im = held[m, 0, rows, :], held[m, 1, rows, :]
        d_re, d_im = prev[path, m, 0], prev[path, m, 1]
        den = light + shift
        p_re, p_im = g_re / den, g_im / den
        pre_ref[m, 0, to, :] = p_re
        pre_ref[m, 1, to, :] = p_im
        parts = gather_parts(m, path)
        line, chunk, send, recv = parts[0]
        walk = line.gather(chunk, send, recv)
        next(walk, None)
        terms = (
            g_re * p_re + g_im * p_im,
            g_re * d_re + g_im * d_im,
            light * (p_re * p_re + p_im * p_im),
            light * (p_re * d_re + p_im * d_im),
            light * (d_re * d_re + d_im * d_im),
        )
        for k, term in enumerate(terms):
            tile = jnp.sum(fold_lanes(term), axis=0, keepdims=True)
            row = 5 * m + k
            sums_in[row : row + 1, :] = tile if path == 0 else sums_in[row : row + 1, :] + tile
        yield
        yield from walk
        line, chunk, send, recv = parts[1]
        yield from line.gather(chunk, send, recv)
        home(m, path).start()

    def run(streams):
        streams = list(streams)
        while streams:
            alive = []
            for stream in streams:
                try:
                    next(stream)
                    alive.append(stream)
                except StopIteration:
                    pass
            streams = alive

    sums_in[...] = jnp.zeros_like(sums_in)
    run([scatter(modes, 0), scatter(modes, 1)])
    illum_done()
    shift = shift_value()

    def lagged(stream, lag):
        for _ in range(lag):
            yield
        yield from stream

    run(lagged(mode(m, path, shift), 2 * m) for m in range(modes) for path in range(2))

    for copy in broadcast(sums_in, sums_all, 1):
        copy.start()
    sums_all[0] = sums_in[...]
    for copy in broadcast(sums_in, sums_all, 1):
        copy.wait_recv()
    sums_ref[...] = jnp.sum(sums_all[...], axis=0)

    for m in range(modes):
        for path in range(2):
            home(m, path).wait_recv()
    for m in items:
        give(m).wait_send()
        for path in range(2):
            for line, chunk, slot, send, recv in scatter_parts(m, path):
                line.scatter_end(chunk, slot, send, recv)
            if m < modes:
                for line, chunk, send, recv in gather_parts(m, path):
                    line.gather_end(chunk, send, recv)
                home(m, path).wait_send()
    for which, src, dst in ((0, shift_in, shift_all), (1, sums_in, sums_all)):
        for copy in broadcast(src, dst, which):
            copy.wait_send()


def reduce_grads(part, illum, direction):
    modes, _, width, _ = part.shape
    shape = split_lines(lax.axis_size("grp"))
    outer, inner, cores = shape
    count = outer * inner * cores
    half = width // cores // 2
    own = half // (outer * inner)
    sizes = [(inner, half // inner), (outer, own), (outer, half // outer), (inner, own)]
    back_sizes = [outer, inner, inner, outer]
    sum_rows = -(-5 * modes // 8) * 8
    lanes = min(128, width)
    dma = pltpu.SemaphoreType.DMA
    f32 = jnp.float32
    scratch = [
        pltpu.VMEM((modes, 2, width // cores, width), f32),
        pltpu.VMEM((1, width // cores, width), f32),
        pltpu.VMEM((2, modes, 2, own, width), f32),
        pltpu.VMEM((8, lanes), f32),
        pltpu.VMEM((count, 8, lanes), f32),
        pltpu.VMEM((sum_rows, lanes), f32),
        pltpu.VMEM((count, sum_rows, lanes), f32),
    ]
    scratch += [pltpu.VMEM((modes, n + 1, 2, rows, width), f32) for n, rows in sizes]
    scratch += [pltpu.VMEM((n + 1, 1, rows, width), f32) for n, rows in sizes]
    scratch += [dma((modes + 1,)), dma((modes + 1,))]
    scratch += [dma((modes, n)) for n, _ in sizes] + [dma((modes, n + 1)) for n, _ in sizes]
    scratch += [dma((modes, 2, n)) for n in back_sizes] + [dma((modes, n)) for n in back_sizes]
    scratch += [dma((n,)) for n, _ in sizes] + [dma((n + 1,)) for n, _ in sizes]
    scratch += [dma((modes, 2)), dma((modes, 2)), dma((2, modes)), dma((2, count)), dma((2, count))]
    vmem = pl.BlockSpec(memory_space=pltpu.VMEM)
    return pl.pallas_call(
        functools.partial(reduce_kernel, shape, modes, width),
        in_specs=[vmem, vmem, pl.BlockSpec(memory_space=pl.ANY)],
        out_specs=[vmem, vmem],
        out_shape=[
            jax.ShapeDtypeStruct(part.shape, f32),
            jax.ShapeDtypeStruct((sum_rows, lanes), f32),
        ],
        scratch_shapes=scratch,
        compiler_params=pltpu.CompilerParams(collective_id=0, has_side_effects=True, vmem_limit_bytes=VMEM_LIMIT),
        name="reduce",
    )(part, illum[None], direction)


def finish_kernel(norm_ref, sums_ref, pre_ref, probe_ref, dir_ref, new_probe, new_dir, new_norm):
    mode = pl.program_id(0)
    pixels = float(new_probe.shape[3] ** 2)
    index = lax.broadcasted_iota(jnp.int32, sums_ref.shape, 0)

    def mean(k):
        return jnp.sum(jnp.where(index == 5 * mode + k, sums_ref[...], 0.0)) / pixels

    norm, cross, light, light_cross, light_prev = (mean(k) for k in range(5))
    new_norm[mode] = norm
    beta = norm / norm_ref[mode]
    upper = norm + beta * cross
    lower = light + beta * (2.0 * light_cross + beta * light_prev)
    alpha = upper / (lower + 1.0)
    for part in range(2):
        step = pre_ref[0, part] + beta * dir_ref[part, 0]
        new_dir[part, 0] = step
        new_probe[part, 0] = probe_ref[part, 0] + alpha * step


def finish(prev_norm, sums, pre, probe, direction):
    modes, width = probe.shape[1], probe.shape[2]
    rows = min(128, width)
    block = pl.BlockSpec((2, 1, rows, width), lambda m, r: (0, m, r, 0))
    smem = pl.BlockSpec(memory_space=pltpu.SMEM)
    return pl.pallas_call(
        finish_kernel,
        grid=(modes, width // rows),
        in_specs=[
            smem,
            whole(sums.shape),
            pl.BlockSpec((1, 2, rows, width), lambda m, r: (m, 0, r, 0)),
            block,
            block,
        ],
        out_specs=[block, block, smem],
        out_shape=[
            jax.ShapeDtypeStruct(probe.shape, jnp.float32),
            jax.ShapeDtypeStruct(probe.shape, jnp.float32),
            jax.ShapeDtypeStruct((modes,), jnp.float32),
        ],
        compiler_params=pltpu.CompilerParams(
            dimension_semantics=("arbitrary", "arbitrary"), vmem_limit_bytes=32 * 1024 * 1024
        ),
        name="finish",
    )(prev_norm, sums, pre, probe, direction)


def sum_over_modes(local_sum):
    if lax.axis_size("mode") != 2:
        return lax.psum(local_sum, "mode")
    return local_sum + lax.ppermute(local_sum, "mode", [(0, 1), (1, 0)])


def on_device(probe, prev_direction, prev_norm, object_tile, offsets, amplitude):
    width = probe.shape[2]
    modes = probe.shape[1]
    positions = amplitude.shape[0]
    base = base_table(width)
    illum = jnp.zeros((width, width), jnp.float32)
    patches, kept = [], []
    for index in range(positions):
        patch = lax.dynamic_slice(
            object_tile, (jnp.int32(0), offsets[index, 0], offsets[index, 1]), (2, width, width)
        )
        patches.append(patch)
        wave, exits, local_sum = forward(base, probe, patch)
        total = sum_over_modes(local_sum)
        kept.append((wave, exits, total))
        wide = patch.astype(jnp.float32)
        illum = illum + wide[0] * wide[0] + wide[1] * wide[1]
    grad = None
    for index in range(positions - 1):
        wave, exits, total = kept[index]
        grad = backward(base, total, amplitude, index, wave, exits, patches[index], grad, 0, modes)
    wave, exits, total = kept[-1]
    part = backward(base, total, amplitude, positions - 1, wave, exits, patches[-1], grad, 0, modes)
    pre, sums = reduce_grads(part, illum, prev_direction)
    return tuple(finish(prev_norm, sums, pre, probe, prev_direction))


def solution(mesh):
    return jax.shard_map(
        on_device,
        mesh=mesh,
        in_specs=(
            P(None, "mode", None, None),
            P(None, "mode", None, None),
            P("mode"),
            P(None, "grp", None),
            P("grp", None),
            P("grp", None, None),
        ),
        out_specs=(P(None, "mode", None, None), P(None, "mode", None, None), P("mode")),
        check_vma=False,
    )
```

```python
import functools
import math

import jax
import jax.numpy as jnp
from jax import lax
from jax.experimental import pallas as pl
from jax.experimental.pallas import tpu as pltpu
from jax.sharding import PartitionSpec as P

MESH = pl.DeviceIdType.MESH
VMEM_LIMIT = 60 * 1024 * 1024
FRONT_LIMIT = 67043328


def base_table(width):
    index = jnp.arange(width, dtype=jnp.int32)
    product = index[:, None] * index[None, :] % width
    angle = -2.0 * math.pi / width * product.astype(jnp.float32)
    scale = 1.0 / math.sqrt(width)
    real_part = (jnp.cos(angle) * scale).astype(jnp.bfloat16)
    imag_part = (jnp.sin(angle) * scale).astype(jnp.bfloat16)
    return jnp.stack([real_part, imag_part])


def fold_lanes(block):
    rows, width = block.shape
    lanes = min(128, width)
    acc = jnp.sum(block.reshape(rows // 8, 8, width), axis=0)
    out = acc[:, :lanes]
    for at in range(lanes, width, lanes):
        out = out + acc[:, at : at + lanes]
    return out


class Spot:
    def __init__(self, outer, inner, cores):
        me = lax.axis_index("grp")
        self.me = me
        self.sizes = (outer, inner, cores)
        self.count = outer * inner * cores
        self.core = lax.rem(me, cores)
        self.inner = lax.rem(me // cores, inner)
        self.outer = me // (cores * inner)
        self.stride = {"core": 1, "inner": cores, "outer": cores * inner}

    def at(self, line, step):
        return {"grp": self.me + step * self.stride[line]}

    def partner(self):
        return {"grp": self.me + 1 - 2 * self.core}


def remote(src, dst, send, recv, device):
    return pltpu.make_async_remote_copy(
        src_ref=src, dst_ref=dst, send_sem=send, recv_sem=recv, device_id=device, device_id_type=MESH
    )


class Line:
    def __init__(self, spot, name, length, place):
        self.spot, self.name, self.length, self.place = spot, name, length, place

    def scatter(self, chunk, slots, send, recv):
        size, u = self.length, self.place

        def take(slot, into):
            got = remote(slots.at[slot], slots.at[slot], send.at[0], recv.at[slot], self.spot.at(self.name, 0))
            got.wait_recv()
            into[...] += slots[slot]

        def push(k, step, slot):
            remote(chunk(k), slots.at[slot], send.at[k], recv.at[slot], self.spot.at(self.name, step)).start()

        for step in range(size - 1):
            right, left = size - 1 - step, step

            @pl.when(u < right)
            def _():
                @pl.when(u > 0)
                def _():
                    take(right + 1, chunk(right))

                push(right, 1, right + 1)

            @pl.when(u > left)
            def _():
                @pl.when(u < size - 1)
                def _():
                    take(left, chunk(left))

                push(left, -1, left)

            yield

        @pl.when(u > 0)
        def _():
            take(u + 1, chunk(u))

        @pl.when(u < size - 1)
        def _():
            take(u, chunk(u))

    def scatter_end(self, chunk, slots, send, recv):
        for k in range(self.length):
            @pl.when(self.place != k)
            def _():
                remote(chunk(k), slots.at[0], send.at[k], recv.at[0], self.spot.at(self.name, 0)).wait_send()

    def gather(self, chunk, send, recv):
        size, u = self.length, self.place

        def push(k, way, step):
            remote(chunk(k), chunk(k), send.at[way, k], recv.at[k], self.spot.at(self.name, step)).start()

        def take(k):
            remote(chunk(k), chunk(k), send.at[0, 0], recv.at[k], self.spot.at(self.name, 0)).wait_recv()

        for step in range(size):
            low, high = u - step, u + step

            @pl.when(low >= 0)
            def _():
                if step > 0:
                    take(low)

                @pl.when(u < size - 1)
                def _():
                    push(low, 0, 1)

            @pl.when(high < size)
            def _():
                if step > 0:
                    take(high)

                @pl.when(u > 0)
                def _():
                    push(high, 1, -1)

            if step < size - 1:
                yield

    def gather_end(self, chunk, send, recv):
        size, u = self.length, self.place
        for k in range(size):
            for way in range(2):
                @pl.when((u < size - 1) & (u >= k) if way == 0 else (u > 0) & (u <= k))
                def _():
                    remote(chunk(k), chunk(k), send.at[way, k], recv.at[k], self.spot.at(self.name, 0)).wait_send()


def build_tables(base_ref, plus, minus):
    width = base_ref.shape[1]
    tile = width // 2
    for row in range(2):
        for col in range(2):
            take = (pl.ds(row * tile, tile), pl.ds(col * tile, tile))
            cosine, sine = base_ref[(0, *take)], base_ref[(1, *take)]
            for ref, upper, lower in ((plus, sine, -sine), (minus, -sine, sine)):
                r, c = row * width, col * width
                ref[r : r + tile, c : c + tile] = cosine
                ref[r + tile : r + width, c + tile : c + width] = cosine
                ref[r : r + tile, c + tile : c + width] = upper
                ref[r + tile : r + width, c : c + tile] = lower


def front_kernel(
    peers, base_ref, probe_ref, patch_ref, amp_ref, grad_ref,
    plus, minus, probe, exits, wave, stacked, own, other, load_sem, send_sem, recv_sem,
):
    positions, modes = exits.shape[0], exits.shape[1]
    width = base_ref.shape[1]
    tile = width // 2
    step = min(64, tile)
    f32, bf16 = jnp.float32, jnp.bfloat16
    y = lax.axis_index("mode")

    barrier = pltpu.get_barrier_semaphore()
    for k in range(1, peers):
        pl.semaphore_signal(barrier, inc=1, device_id={"mode": lax.rem(y + k, peers)}, device_id_type=MESH)

    def load(m):
        return pltpu.make_async_copy(probe_ref.at[:, m], probe.at[m], load_sem.at[m])

    for m in range(modes):
        load(m).start()
    build_tables(base_ref, plus, minus)
    if peers > 1:
        pl.semaphore_wait(barrier, peers - 1)

    def swap(p, t, k):
        rows = pl.ds(t * tile, tile)
        return remote(
            own.at[p, rows], other.at[k - 1, p, rows], send_sem.at[k - 1, p, t], recv_sem.at[k - 1, p, t],
            {"mode": lax.rem(y + k, peers)},
        )

    def put(half, m, rows):
        for col in range(2):
            for part in range(2):
                block = half[:, (2 * col + part) * tile : (2 * col + part + 1) * tile]
                stacked[m, pl.ds(rows * width + part * tile, tile), col * tile : (col + 1) * tile] = block

    def leave(p, m):
        def body(i, carry):
            rows = pl.ds(pl.multiple_of(i * step, step), step)
            for col in range(2):
                at = pl.ds(col * tile, tile)
                obj_re = patch_ref[p, 0, rows, at].astype(f32)
                obj_im = patch_ref[p, 1, rows, at].astype(f32)
                pro_re, pro_im = probe[m, 0, rows, at], probe[m, 1, rows, at]
                exits[p, m, rows, 2 * col * tile : (2 * col + 1) * tile] = (pro_re * obj_re - pro_im * obj_im).astype(bf16)
                exits[p, m, rows, (2 * col + 1) * tile : (2 * col + 2) * tile] = (pro_re * obj_im + pro_im * obj_re).astype(bf16)
            return carry

        lax.fori_loop(0, width // step, body, 0)

    def forward(p, carry):
        def first(m, carry):
            @pl.when(p == 0)
            def _():
                load(m).wait()

            leave(p, m)
            half = jnp.dot(exits[p, m], plus[...], preferred_element_type=f32).astype(bf16)
            for rows in range(2):
                put(half[rows * tile : (rows + 1) * tile], m, rows)
            return carry

        lax.fori_loop(0, modes, first, 0)
        for t in range(2):
            rows = pl.ds(t * tile, tile)

            def second(m, carry):
                out = jnp.dot(minus[t * width : (t + 1) * width, :], stacked[m], preferred_element_type=f32)
                real, imag = out[:tile], out[tile:]
                wave[p, m, t, 0] = real
                wave[p, m, t, 1] = imag
                light = real * real + imag * imag
                own[p, rows, :] = jnp.where(m == 0, light, own[p, rows, :] + light)
                return carry

            lax.fori_loop(0, modes, second, 0)
            for k in range(1, peers):
                swap(p, t, k).start()
        return carry

    lax.fori_loop(0, positions, forward, 0)

    def backward(p, carry):
        for t in range(2):
            for k in range(1, peers):
                swap(p, t, k).wait_recv()

            def scale(i, carry):
                rows = pl.ds(pl.multiple_of(t * tile + i * step, step), step)
                total = own[p, rows, :]
                for k in range(peers - 1):
                    total = total + other[k, p, rows, :]
                ratio = amp_ref[p, rows, :].astype(f32) / jnp.sqrt(total + 1.0)
                here = pl.ds(pl.multiple_of(i * step, step), step)

                def fix(m, carry):
                    for part in range(2):
                        wave[p, m, t, part, here, :] = wave[p, m, t, part, here, :] * ratio
                    return carry

                lax.fori_loop(0, modes, fix, 0)
                return carry

            lax.fori_loop(0, tile // step, scale, 0)

            def first(m, carry):
                fixed = [wave[p, m, t, part].astype(bf16) for part in range(2)]
                blocks = [fixed[part][:, col * tile : (col + 1) * tile] for col in range(2) for part in range(2)]
                joined = jnp.concatenate(blocks, axis=1)
                half = jnp.dot(joined, minus[...], preferred_element_type=f32).astype(bf16)
                put(half, m, t)
                return carry

            lax.fori_loop(0, modes, first, 0)

        def second(m, carry):
            for t in range(2):
                rows = pl.ds(t * tile, tile)
                out = jnp.dot(plus[t * width : (t + 1) * width, :], stacked[m], preferred_element_type=f32)
                for col in range(2):
                    at = pl.ds(col * tile, tile)
                    real, imag = out[:tile, col * tile : (col + 1) * tile], out[tile:, col * tile : (col + 1) * tile]
                    obj_re = patch_ref[p, 0, rows, at].astype(f32)
                    obj_im = patch_ref[p, 1, rows, at].astype(f32)
                    diff_re = real - exits[p, m, rows, 2 * col * tile : (2 * col + 1) * tile].astype(f32)
                    diff_im = imag - exits[p, m, rows, (2 * col + 1) * tile : (2 * col + 2) * tile].astype(f32)
                    add_re = obj_re * diff_re + obj_im * diff_im
                    add_im = obj_re * diff_im - obj_im * diff_re
                    grad_ref[m, 0, rows, at] = jnp.where(p == 0, add_re, grad_ref[m, 0, rows, at] + add_re)
                    grad_ref[m, 1, rows, at] = jnp.where(p == 0, add_im, grad_ref[m, 1, rows, at] + add_im)
            return carry

        lax.fori_loop(0, modes, second, 0)
        return carry

    lax.fori_loop(0, positions, backward, 0)
    for p in range(positions):
        for t in range(2):
            for k in range(1, peers):
                swap(p, t, k).wait_send()


def front(base, probe, patches, amplitude):
    modes, width = probe.shape[1], probe.shape[2]
    positions = patches.shape[0]
    peers = lax.axis_size("mode")
    tile = width // 2
    dma = pltpu.SemaphoreType.DMA
    f32, bf16 = jnp.float32, jnp.bfloat16
    vmem = pl.BlockSpec(memory_space=pltpu.VMEM)
    flops = positions * modes * 2 * 16 * width**3
    return pl.pallas_call(
        functools.partial(front_kernel, peers),
        in_specs=[vmem, pl.BlockSpec(memory_space=pl.ANY), vmem, vmem],
        out_specs=vmem,
        out_shape=jax.ShapeDtypeStruct((modes, 2, width, width), f32),
        scratch_shapes=[
            pltpu.VMEM((2 * width, 2 * width), bf16),
            pltpu.VMEM((2 * width, 2 * width), bf16),
            pltpu.VMEM((modes, 2, width, width), f32),
            pltpu.VMEM((positions, modes, width, 2 * width), bf16),
            pltpu.VMEM((positions, modes, 2, 2, tile, width), f32),
            pltpu.VMEM((modes, 2 * width, width), bf16),
            pltpu.VMEM((positions, width, width), f32),
            pltpu.VMEM((max(peers - 1, 1), positions, width, width), f32),
            dma((modes,)),
            dma((max(peers - 1, 1), positions, 2)),
            dma((max(peers - 1, 1), positions, 2)),
        ],
        compiler_params=pltpu.CompilerParams(collective_id=1, has_side_effects=True, vmem_limit_bytes=FRONT_LIMIT),
        cost_estimate=pl.CostEstimate(flops=flops, bytes_accessed=0, transcendentals=0),
        name="front",
    )(base, probe, patches, amplitude)


def split_lines(cores_total):
    cores = 2 if cores_total % 2 == 0 else 1
    chips = cores_total // cores
    inner = 1
    while inner * inner * 2 <= chips and chips % (inner * 2) == 0:
        inner *= 2
    inner = inner if inner * inner <= chips else inner // 2
    return chips // inner, inner, cores


class Shares:
    def __init__(self, spot, width):
        outer, inner, cores = spot.sizes
        self.part = width // cores
        self.half = self.part // 2
        self.own = self.half // (outer * inner)
        self.base = (spot.core * self.part, spot.core * self.part + self.half)
        a_big, b_big = self.half // inner, self.half // outer
        self.big = (a_big, b_big)
        self.first = ("inner", "outer")
        place = {"inner": spot.inner, "outer": spot.outer}
        size = {"inner": inner, "outer": outer}
        self.lines = tuple(Line(spot, name, size[name], place[name]) for name in ("inner", "outer"))
        self.offset = (
            spot.inner * a_big + spot.outer * self.own,
            spot.outer * b_big + spot.inner * self.own,
        )
        self.group = (spot.inner * a_big, spot.outer * b_big)

    def order(self, path):
        return (self.lines[0], self.lines[1]) if path == 0 else (self.lines[1], self.lines[0])


def rows_at(ref, start, count):
    return ref.at[:, pl.ds(pl.multiple_of(start, 8), count), :]


def reduce_kernel(
    shape, modes, width, grad_ref, illum_ref, dir_ref, pre_ref, sums_ref,
    held, held_i, prev, shift_in, shift_all, sums_in, sums_all, *rest,
):
    outer, inner, cores = shape
    spot = Spot(outer, inner, cores)
    share = Shares(spot, width)
    (slots, islots, core_s, core_r, sc_s, sc_r, ga_s, ga_r, isc_s, isc_r, back_s, back_r, dir_sem, bc_s, bc_r) = (
        rest[0:4], rest[4:8], *rest[8:10], rest[10:14], rest[14:18], rest[18:22], rest[22:26],
        rest[26:30], rest[30:34], *rest[34:],
    )
    me, count = spot.me, spot.count
    pixels = float(width * width)

    barrier = pltpu.get_barrier_semaphore()
    for step in range(1, count):
        pl.semaphore_signal(barrier, inc=1, device_id={"grp": lax.rem(me + step, count)}, device_id_type=MESH)

    loads = []
    for path in range(2):
        start = pl.multiple_of(share.base[path] + share.offset[path], 8)
        for m in range(modes):
            load = pltpu.make_async_copy(
                dir_ref.at[:, m, pl.ds(start, share.own), :], prev.at[path, m], dir_sem.at[path, m]
            )
            load.start()
            loads.append(load)
    pl.semaphore_wait(barrier, count - 1)

    def core_send(src, dst, item):
        return remote(src, dst, core_s.at[item], core_r.at[item], spot.partner())

    def partial(m):
        return grad_ref.at[m] if m < modes else illum_ref

    def keep(m):
        return held.at[m] if m < modes else held_i

    def give(m):
        other = (1 - spot.core) * share.part
        return core_send(rows_at(partial(m), other, share.part), keep(m), m)

    items = [modes] + list(range(modes))
    for m in items:
        give(m).start()

    def pair(m, path):
        if m < modes:
            one, two = 2 * path, 2 * path + 1
            return [(slots[k].at[m], sc_s[k].at[m], sc_r[k].at[m]) for k in (one, two)]
        return [(islots[k], isc_s[k], isc_r[k]) for k in (2 * path, 2 * path + 1)]

    def scatter_parts(m, path):
        first, second = share.order(path)
        at = path * share.half
        top = lambda k: rows_at(keep(m), at + k * share.big[path], share.big[path])
        low = lambda k: rows_at(keep(m), at + share.group[path] + k * share.own, share.own)
        return [(line, chunk) + sems for line, chunk, sems in zip((first, second), (top, low), pair(m, path))]

    def gather_parts(m, path):
        second, first = share.order(path)
        base = share.base[path]
        low = lambda k: rows_at(pre_ref.at[m], base + share.group[path] + k * share.own, share.own)
        top = lambda k: rows_at(pre_ref.at[m], base + k * share.big[path], share.big[path])
        sems = [(ga_s[k].at[m], ga_r[k].at[m]) for k in (2 * path, 2 * path + 1)]
        return [(line, chunk) + pairs for line, chunk, pairs in zip((first, second), (low, top), sems)]

    def home(m, path):
        block = rows_at(pre_ref.at[m], share.base[path], share.half)
        return remote(block, block, back_s.at[m, path], back_r.at[m, path], spot.partner())

    def broadcast(src, dst, which):
        copies = []
        for step in range(1, count):
            to = lax.rem(me + step, count)
            copies.append(remote(src, dst.at[step], bc_s.at[which, step], bc_r.at[which, step], {"grp": to}))
        return copies

    def own_illum(path):
        at = pl.multiple_of(path * share.half + share.offset[path], 8)
        return held_i[0, pl.ds(at, share.own), :]

    def scatter(m, path):
        if path == 0:
            give(m).wait_recv()
            held_m, mine = keep(m), partial(m)
            step = 32 if share.part % 32 == 0 else share.part

            def add(i, carry):
                rows = pl.ds(pl.multiple_of(i * step, 8), step)
                held_m[:, rows, :] += mine[:, pl.ds(pl.multiple_of(spot.core * share.part + i * step, 8), step), :]
                return carry

            lax.fori_loop(0, share.part // step, add, 0)
        for line, chunk, slot, send, recv in scatter_parts(m, path):
            yield from line.scatter(chunk, slot, send, recv)

    def illum_done():
        tile = fold_lanes(own_illum(0)) + fold_lanes(own_illum(1))
        shift_in[...] = tile
        for copy in broadcast(shift_in, shift_all, 0):
            copy.start()
        shift_all[0] = tile

    def shift_value():
        for copy in broadcast(shift_in, shift_all, 0):
            copy.wait_recv()
        return jnp.sum(shift_all[...]) / pixels

    def mode(m, path, shift):
        yield from scatter(m, path)
        at = pl.multiple_of(path * share.half + share.offset[path], 8)
        rows = pl.ds(at, share.own)
        to = pl.ds(pl.multiple_of(share.base[path] + share.offset[path], 8), share.own)
        light = own_illum(path)
        loads[path * modes + m].wait()
        g_re, g_im = held[m, 0, rows, :], held[m, 1, rows, :]
        d_re, d_im = prev[path, m, 0], prev[path, m, 1]
        den = light + shift
        p_re, p_im = g_re / den, g_im / den
        pre_ref[m, 0, to, :] = p_re
        pre_ref[m, 1, to, :] = p_im
        parts = gather_parts(m, path)
        line, chunk, send, recv = parts[0]
        walk = line.gather(chunk, send, recv)
        next(walk, None)
        terms = (
            g_re * p_re + g_im * p_im,
            g_re * d_re + g_im * d_im,
            light * (p_re * p_re + p_im * p_im),
            light * (p_re * d_re + p_im * d_im),
            light * (d_re * d_re + d_im * d_im),
        )
        for k, term in enumerate(terms):
            tile = jnp.sum(fold_lanes(term), axis=0, keepdims=True)
            row = 5 * m + k
            sums_in[row : row + 1, :] = tile if path == 0 else sums_in[row : row + 1, :] + tile
        yield
        yield from walk
        line, chunk, send, recv = parts[1]
        yield from line.gather(chunk, send, recv)
        home(m, path).start()

    def run(streams):
        streams = list(streams)
        while streams:
            alive = []
            for stream in streams:
                try:
                    next(stream)
                    alive.append(stream)
                except StopIteration:
                    pass
            streams = alive

    sums_in[...] = jnp.zeros_like(sums_in)
    run([scatter(modes, 0), scatter(modes, 1)])
    illum_done()
    shift = shift_value()

    def lagged(stream, lag):
        for _ in range(lag):
            yield
        yield from stream

    run(lagged(mode(m, path, shift), 2 * m) for m in range(modes) for path in range(2))

    for copy in broadcast(sums_in, sums_all, 1):
        copy.start()
    sums_all[0] = sums_in[...]
    for copy in broadcast(sums_in, sums_all, 1):
        copy.wait_recv()
    sums_ref[...] = jnp.sum(sums_all[...], axis=0)

    for m in range(modes):
        for path in range(2):
            home(m, path).wait_recv()
    for m in items:
        give(m).wait_send()
        for path in range(2):
            for line, chunk, slot, send, recv in scatter_parts(m, path):
                line.scatter_end(chunk, slot, send, recv)
            if m < modes:
                for line, chunk, send, recv in gather_parts(m, path):
                    line.gather_end(chunk, send, recv)
                home(m, path).wait_send()
    for which, src, dst in ((0, shift_in, shift_all), (1, sums_in, sums_all)):
        for copy in broadcast(src, dst, which):
            copy.wait_send()


def reduce_grads(part, illum, direction):
    modes, _, width, _ = part.shape
    shape = split_lines(lax.axis_size("grp"))
    outer, inner, cores = shape
    count = outer * inner * cores
    half = width // cores // 2
    own = half // (outer * inner)
    sizes = [(inner, half // inner), (outer, own), (outer, half // outer), (inner, own)]
    back_sizes = [outer, inner, inner, outer]
    sum_rows = -(-5 * modes // 8) * 8
    lanes = min(128, width)
    dma = pltpu.SemaphoreType.DMA
    f32 = jnp.float32
    scratch = [
        pltpu.VMEM((modes, 2, width // cores, width), f32),
        pltpu.VMEM((1, width // cores, width), f32),
        pltpu.VMEM((2, modes, 2, own, width), f32),
        pltpu.VMEM((8, lanes), f32),
        pltpu.VMEM((count, 8, lanes), f32),
        pltpu.VMEM((sum_rows, lanes), f32),
        pltpu.VMEM((count, sum_rows, lanes), f32),
    ]
    scratch += [pltpu.VMEM((modes, n + 1, 2, rows, width), f32) for n, rows in sizes]
    scratch += [pltpu.VMEM((n + 1, 1, rows, width), f32) for n, rows in sizes]
    scratch += [dma((modes + 1,)), dma((modes + 1,))]
    scratch += [dma((modes, n)) for n, _ in sizes] + [dma((modes, n + 1)) for n, _ in sizes]
    scratch += [dma((modes, 2, n)) for n in back_sizes] + [dma((modes, n)) for n in back_sizes]
    scratch += [dma((n,)) for n, _ in sizes] + [dma((n + 1,)) for n, _ in sizes]
    scratch += [dma((modes, 2)), dma((modes, 2)), dma((2, modes)), dma((2, count)), dma((2, count))]
    vmem = pl.BlockSpec(memory_space=pltpu.VMEM)
    return pl.pallas_call(
        functools.partial(reduce_kernel, shape, modes, width),
        in_specs=[vmem, vmem, pl.BlockSpec(memory_space=pl.ANY)],
        out_specs=[vmem, vmem],
        out_shape=[
            jax.ShapeDtypeStruct(part.shape, f32),
            jax.ShapeDtypeStruct((sum_rows, lanes), f32),
        ],
        scratch_shapes=scratch,
        compiler_params=pltpu.CompilerParams(collective_id=0, has_side_effects=True, vmem_limit_bytes=VMEM_LIMIT),
        name="reduce",
    )(part, illum[None], direction)


def finish_kernel(norm_ref, sums_ref, pre_ref, probe_ref, dir_ref, new_probe, new_dir, new_norm):
    mode = pl.program_id(0)
    pixels = float(new_probe.shape[3] ** 2)
    index = lax.broadcasted_iota(jnp.int32, sums_ref.shape, 0)

    def mean(k):
        return jnp.sum(jnp.where(index == 5 * mode + k, sums_ref[...], 0.0)) / pixels

    norm, cross, light, light_cross, light_prev = (mean(k) for k in range(5))
    new_norm[mode] = norm
    beta = norm / norm_ref[mode]
    upper = norm + beta * cross
    lower = light + beta * (2.0 * light_cross + beta * light_prev)
    alpha = upper / (lower + 1.0)
    for part in range(2):
        step = pre_ref[0, part] + beta * dir_ref[part, 0]
        new_dir[part, 0] = step
        new_probe[part, 0] = probe_ref[part, 0] + alpha * step


def finish(prev_norm, sums, pre, probe, direction):
    modes, width = probe.shape[1], probe.shape[2]
    rows = min(128, width)
    block = pl.BlockSpec((2, 1, rows, width), lambda m, r: (0, m, r, 0))
    smem = pl.BlockSpec(memory_space=pltpu.SMEM)
    return pl.pallas_call(
        finish_kernel,
        grid=(modes, width // rows),
        in_specs=[
            smem,
            whole(sums.shape),
            pl.BlockSpec((1, 2, rows, width), lambda m, r: (m, 0, r, 0)),
            block,
            block,
        ],
        out_specs=[block, block, smem],
        out_shape=[
            jax.ShapeDtypeStruct(probe.shape, jnp.float32),
            jax.ShapeDtypeStruct(probe.shape, jnp.float32),
            jax.ShapeDtypeStruct((modes,), jnp.float32),
        ],
        compiler_params=pltpu.CompilerParams(
            dimension_semantics=("arbitrary", "arbitrary"), vmem_limit_bytes=32 * 1024 * 1024
        ),
        name="finish",
    )(prev_norm, sums, pre, probe, direction)


def whole(shape):
    return pl.BlockSpec(shape, lambda *_: (0,) * len(shape))


def on_device(probe, prev_direction, prev_norm, object_tile, offsets, amplitude):
    width = probe.shape[2]
    positions = amplitude.shape[0]
    zero = jnp.int32(0)
    patches = jnp.stack(
        [
            lax.dynamic_slice(object_tile, (zero, offsets[k, 0], offsets[k, 1]), (2, width, width))
            for k in range(positions)
        ]
    )
    wide = patches.astype(jnp.float32)
    illum = jnp.sum(wide * wide, axis=(0, 1))
    part = front(base_table(width), probe, patches, amplitude)
    pre, sums = reduce_grads(part, illum, prev_direction)
    return tuple(finish(prev_norm, sums, pre, probe, prev_direction))


def solution(mesh):
    return jax.shard_map(
        on_device,
        mesh=mesh,
        in_specs=(
            P(None, "mode", None, None),
            P(None, "mode", None, None),
            P("mode"),
            P(None, "grp", None),
            P("grp", None),
            P("grp", None, None),
        ),
        out_specs=(P(None, "mode", None, None), P(None, "mode", None, None), P("mode")),
        check_vma=False,
    )
```

```python
import functools
import math

import jax
import jax.numpy as jnp
from jax import lax
from jax.experimental import pallas as pl
from jax.experimental.pallas import tpu as pltpu
from jax.sharding import PartitionSpec as P

MESH = pl.DeviceIdType.MESH
VMEM_LIMIT = 60 * 1024 * 1024
FRONT_LIMIT = 67043328
REDUCE_LIMIT = 33 * 1024 * 1024
FINISH_LIMIT = 18 * 1024 * 1024
ORDERS = {
    (4, 2, 2, 4): (
        (
            0, 1, 0, 0, 2, 0, 0, 3, 2, 1, 0, 1, 1, 2, 1, 0, 0, 1, 2, 1, 3, 0, 0, 1, 3, 1, 0, 0, 3,
            1, 3, 0, 1, 2, 3, 2, 0, 3, 2, 1, 3, 2, 3, 3, 2, 2, 0, 3, 3, 1, 1, 1, 3, 2, 2, 3, 2, 2,
            3, 2,
        ),
        (
            0, 1, 0, 0, 1, 0, 0, 0, 2, 1, 2, 1, 0, 3, 1, 0, 1, 1, 3, 0, 3, 1, 3, 2, 0, 3, 1, 3, 2,
            0, 3, 0, 2, 1, 1, 2, 3, 2, 1, 3, 2, 0, 2, 1, 2, 3, 0, 0, 2, 1, 2, 3, 1, 2, 2, 3, 3, 2,
            3, 3,
        ),
    ),
}


def base_table(width):
    index = jnp.arange(width, dtype=jnp.int32)
    product = index[:, None] * index[None, :] % width
    angle = -2.0 * math.pi / width * product.astype(jnp.float32)
    scale = 1.0 / math.sqrt(width)
    real_part = (jnp.cos(angle) * scale).astype(jnp.bfloat16)
    imag_part = (jnp.sin(angle) * scale).astype(jnp.bfloat16)
    return jnp.stack([real_part, imag_part])


def fold_lanes(block):
    rows, width = block.shape
    lanes = min(128, width)
    acc = jnp.sum(block.reshape(rows // 8, 8, width), axis=0)
    out = acc[:, :lanes]
    for at in range(lanes, width, lanes):
        out = out + acc[:, at : at + lanes]
    return out


class Spot:
    def __init__(self, outer, inner, cores):
        me = lax.axis_index("grp")
        self.me = me
        self.sizes = (outer, inner, cores)
        self.count = outer * inner * cores
        self.core = lax.rem(me, cores)
        self.inner = lax.rem(me // cores, inner)
        self.outer = me // (cores * inner)
        self.stride = {"core": 1, "inner": cores, "outer": cores * inner}

    def at(self, line, step):
        return {"grp": self.me + step * self.stride[line]}

    def partner(self):
        return {"grp": self.me + 1 - 2 * self.core}


def remote(src, dst, send, recv, device):
    return pltpu.make_async_remote_copy(
        src_ref=src, dst_ref=dst, send_sem=send, recv_sem=recv, device_id=device, device_id_type=MESH
    )


class Line:
    def __init__(self, spot, name, length, place):
        self.spot, self.name, self.length, self.place = spot, name, length, place

    def scatter(self, chunk, slots, send, recv):
        size, u = self.length, self.place

        def take(slot, into):
            got = remote(slots.at[slot], slots.at[slot], send.at[0], recv.at[slot], self.spot.at(self.name, 0))
            got.wait_recv()
            into[...] += slots[slot]

        def push(k, step, slot):
            remote(chunk(k), slots.at[slot], send.at[k], recv.at[slot], self.spot.at(self.name, step)).start()

        for step in range(size - 1):
            right, left = size - 1 - step, step

            @pl.when(u < right)
            def _():
                @pl.when(u > 0)
                def _():
                    take(right + 1, chunk(right))

                push(right, 1, right + 1)

            if size > 2:
                yield

            @pl.when(u > left)
            def _():
                @pl.when(u < size - 1)
                def _():
                    take(left, chunk(left))

                push(left, -1, left)

            yield

        @pl.when(u > 0)
        def _():
            take(u + 1, chunk(u))

        @pl.when(u < size - 1)
        def _():
            take(u, chunk(u))

    def scatter_end(self, chunk, slots, send, recv):
        for k in range(self.length):
            @pl.when(self.place != k)
            def _():
                remote(chunk(k), slots.at[0], send.at[k], recv.at[0], self.spot.at(self.name, 0)).wait_send()

    def gather(self, chunk, send, recv):
        size, u = self.length, self.place

        def push(k, way, step):
            remote(chunk(k), chunk(k), send.at[way, k], recv.at[k], self.spot.at(self.name, step)).start()

        def take(k):
            remote(chunk(k), chunk(k), send.at[0, 0], recv.at[k], self.spot.at(self.name, 0)).wait_recv()

        for step in range(size):
            low, high = u - step, u + step

            @pl.when(low >= 0)
            def _():
                if step > 0:
                    take(low)

                @pl.when(u < size - 1)
                def _():
                    push(low, 0, 1)

            if size > 2 and step > 0:
                yield

            @pl.when(high < size)
            def _():
                if step > 0:
                    take(high)

                @pl.when(u > 0)
                def _():
                    push(high, 1, -1)

            if step < size - 1:
                yield

    def gather_end(self, chunk, send, recv):
        size, u = self.length, self.place
        for k in range(size):
            for way in range(2):
                @pl.when((u < size - 1) & (u >= k) if way == 0 else (u > 0) & (u <= k))
                def _():
                    remote(chunk(k), chunk(k), send.at[way, k], recv.at[k], self.spot.at(self.name, 0)).wait_send()


def build_tables(base_ref, plus, minus):
    width = base_ref.shape[1]
    tile = width // 2
    for row in range(2):
        for col in range(2):
            take = (pl.ds(row * tile, tile), pl.ds(col * tile, tile))
            cosine, sine = base_ref[(0, *take)], base_ref[(1, *take)]
            for ref, upper, lower in ((plus, sine, -sine), (minus, -sine, sine)):
                r, c = row * width, col * width
                ref[r : r + tile, c : c + tile] = cosine
                ref[r + tile : r + width, c + tile : c + width] = cosine
                ref[r : r + tile, c + tile : c + width] = upper
                ref[r + tile : r + width, c : c + tile] = lower


def front_kernel(
    peers, shape, base_ref, probe_ref, patch_ref, amp_ref, grad_ref, light_ref, total_ref,
    plus, minus, probe, exits, wave, stacked, own, other, load_sem, send_sem, recv_sem,
    lit, held, tile_in, tile_all, *rest,
):
    slots, sc_s, sc_r, (core_s, core_r, bc_s, bc_r) = rest[0:4], rest[4:8], rest[8:12], rest[12:]
    spot = Spot(*shape)
    positions, modes = exits.shape[0], exits.shape[1]
    width = base_ref.shape[1]
    tile = width // 2
    step = min(64, tile)
    f32, bf16 = jnp.float32, jnp.bfloat16
    y = lax.axis_index("mode")

    barrier = pltpu.get_barrier_semaphore()
    for k in range(1, peers):
        pl.semaphore_signal(barrier, inc=1, device_id={"mode": lax.rem(y + k, peers)}, device_id_type=MESH)
    for k in range(1, spot.count):
        to = lax.rem(spot.me + k, spot.count)
        pl.semaphore_signal(barrier, inc=1, device_id={"grp": to}, device_id_type=MESH)

    def load(m):
        return pltpu.make_async_copy(probe_ref.at[:, m], probe.at[m], load_sem.at[m])

    for m in range(modes):
        load(m).start()
    build_tables(base_ref, plus, minus)
    share = Shares(spot, width)
    pl.semaphore_wait(barrier, peers - 1 + spot.count - 1)

    def swap(p, t, k):
        rows = pl.ds(t * tile, tile)
        return remote(
            own.at[p, rows], other.at[k - 1, p, rows], send_sem.at[k - 1, p, t], recv_sem.at[k - 1, p, t],
            {"mode": lax.rem(y + k, peers)},
        )

    def put(half, m, rows):
        for col in range(2):
            for part in range(2):
                block = half[:, (2 * col + part) * tile : (2 * col + part + 1) * tile]
                stacked[m, pl.ds(rows * width + part * tile, tile), col * tile : (col + 1) * tile] = block

    def leave(p, m):
        def body(i, carry):
            rows = pl.ds(pl.multiple_of(i * step, step), step)
            for col in range(2):
                at = pl.ds(col * tile, tile)
                obj_re = patch_ref[p, 0, rows, at].astype(f32)
                obj_im = patch_ref[p, 1, rows, at].astype(f32)
                pro_re, pro_im = probe[m, 0, rows, at], probe[m, 1, rows, at]
                exits[p, m, rows, 2 * col * tile : (2 * col + 1) * tile] = (pro_re * obj_re - pro_im * obj_im).astype(bf16)
                exits[p, m, rows, (2 * col + 1) * tile : (2 * col + 2) * tile] = (pro_re * obj_im + pro_im * obj_re).astype(bf16)
            return carry

        lax.fori_loop(0, width // step, body, 0)

    def forward(p, carry):
        def first(m, carry):
            @pl.when(p == 0)
            def _():
                load(m).wait()

            leave(p, m)
            half = jnp.dot(exits[p, m], plus[...], preferred_element_type=f32).astype(bf16)
            for rows in range(2):
                put(half[rows * tile : (rows + 1) * tile], m, rows)
            return carry

        lax.fori_loop(0, modes, first, 0)
        for t in range(2):
            rows = pl.ds(t * tile, tile)

            def second(m, carry):
                out = jnp.dot(minus[t * width : (t + 1) * width, :], stacked[m], preferred_element_type=f32)
                real, imag = out[:tile], out[tile:]
                wave[p, m, t, 0] = real
                wave[p, m, t, 1] = imag
                light = real * real + imag * imag
                own[p, rows, :] = jnp.where(m == 0, light, own[p, rows, :] + light)
                return carry

            lax.fori_loop(0, modes, second, 0)
            for k in range(1, peers):
                swap(p, t, k).start()
        return carry

    lax.fori_loop(0, positions, forward, 0)

    def give():
        away = rows_at(lit, (1 - spot.core) * share.part, share.part)
        return remote(away, held, core_s.at[0], core_r.at[0], spot.partner())

    def shine(i, carry):
        rows = pl.ds(pl.multiple_of(i * step, step), step)
        acc = jnp.zeros((step, width), f32)
        for p in range(positions):
            obj_re, obj_im = patch_ref[p, 0, rows, :].astype(f32), patch_ref[p, 1, rows, :].astype(f32)
            acc = acc + obj_re * obj_re + obj_im * obj_im
        lit[0, rows, :] = acc
        return carry

    def parts(path):
        sems = [(slots[k], sc_s[k], sc_r[k]) for k in (2 * path, 2 * path + 1)]
        return share.scatter_parts(path, held, sems)

    def scatter(path):
        for line, chunk, slot, send, recv in parts(path):
            for _ in line.scatter(chunk, slot, send, recv):
                pass
        block = held[0, pl.ds(pl.multiple_of(share.offset[path], 8), share.own), :]
        light_ref[0] = block
        tile_in[...] = fold_lanes(block)

    def scatter_end(path):
        for line, chunk, slot, send, recv in parts(path):
            line.scatter_end(chunk, slot, send, recv)

    lax.fori_loop(0, width // step, shine, 0)
    give().start()
    give().wait_recv()
    add_rows(held, lit, share.base, share.part)
    per_path(spot, shape[2], scatter)
    for copy in broadcast(spot, tile_in, tile_all, bc_s, bc_r):
        copy.start()
    tile_all[0] = tile_in[...]

    def backward(p, carry):
        for t in range(2):
            for k in range(1, peers):
                swap(p, t, k).wait_recv()

            def scale(i, carry):
                rows = pl.ds(pl.multiple_of(t * tile + i * step, step), step)
                total = own[p, rows, :]
                for k in range(peers - 1):
                    total = total + other[k, p, rows, :]
                ratio = amp_ref[p, rows, :].astype(f32) / jnp.sqrt(total + 1.0)
                here = pl.ds(pl.multiple_of(i * step, step), step)

                def fix(m, carry):
                    for part in range(2):
                        wave[p, m, t, part, here, :] = wave[p, m, t, part, here, :] * ratio
                    return carry

                lax.fori_loop(0, modes, fix, 0)
                return carry

            lax.fori_loop(0, tile // step, scale, 0)

            def first(m, carry):
                fixed = [wave[p, m, t, part].astype(bf16) for part in range(2)]
                blocks = [fixed[part][:, col * tile : (col + 1) * tile] for col in range(2) for part in range(2)]
                joined = jnp.concatenate(blocks, axis=1)
                half = jnp.dot(joined, minus[...], preferred_element_type=f32).astype(bf16)
                put(half, m, t)
                return carry

            lax.fori_loop(0, modes, first, 0)

        def second(m, carry):
            for t in range(2):
                rows = pl.ds(t * tile, tile)
                out = jnp.dot(plus[t * width : (t + 1) * width, :], stacked[m], preferred_element_type=f32)
                for col in range(2):
                    at = pl.ds(col * tile, tile)
                    real, imag = out[:tile, col * tile : (col + 1) * tile], out[tile:, col * tile : (col + 1) * tile]
                    obj_re = patch_ref[p, 0, rows, at].astype(f32)
                    obj_im = patch_ref[p, 1, rows, at].astype(f32)
                    diff_re = real - exits[p, m, rows, 2 * col * tile : (2 * col + 1) * tile].astype(f32)
                    diff_im = imag - exits[p, m, rows, (2 * col + 1) * tile : (2 * col + 2) * tile].astype(f32)
                    add_re = obj_re * diff_re + obj_im * diff_im
                    add_im = obj_re * diff_im - obj_im * diff_re
                    grad_ref[m, 0, rows, at] = jnp.where(p == 0, add_re, grad_ref[m, 0, rows, at] + add_re)
                    grad_ref[m, 1, rows, at] = jnp.where(p == 0, add_im, grad_ref[m, 1, rows, at] + add_im)
            return carry

        lax.fori_loop(0, modes, second, 0)
        return carry

    lax.fori_loop(0, positions, backward, 0)
    for copy in broadcast(spot, tile_in, tile_all, bc_s, bc_r):
        copy.wait()
    total_ref[...] = jnp.sum(tile_all[...], axis=0)
    give().wait_send()
    per_path(spot, shape[2], scatter_end)
    for p in range(positions):
        for t in range(2):
            for k in range(1, peers):
                swap(p, t, k).wait_send()


def front(base, probe, patches, amplitude):
    modes, width = probe.shape[1], probe.shape[2]
    positions = patches.shape[0]
    peers = lax.axis_size("mode")
    tile = width // 2
    dma = pltpu.SemaphoreType.DMA
    f32, bf16 = jnp.float32, jnp.bfloat16
    vmem = pl.BlockSpec(memory_space=pltpu.VMEM)
    shape = split_lines(lax.axis_size("grp"))
    sizes = scatter_sizes(shape, width)
    count, lanes = lax.axis_size("grp"), min(128, width)
    flops = positions * modes * 2 * 16 * width**3
    return pl.pallas_call(
        functools.partial(front_kernel, peers, shape),
        in_specs=[vmem, pl.BlockSpec(memory_space=pl.ANY), vmem, vmem],
        out_specs=[vmem, vmem, vmem],
        out_shape=[
            jax.ShapeDtypeStruct((modes, 2, width, width), f32),
            jax.ShapeDtypeStruct((1, sizes[1][1], width), f32),
            jax.ShapeDtypeStruct((8, lanes), f32),
        ],
        scratch_shapes=[
            pltpu.VMEM((2 * width, 2 * width), bf16),
            pltpu.VMEM((2 * width, 2 * width), bf16),
            pltpu.VMEM((modes, 2, width, width), f32),
            pltpu.VMEM((positions, modes, width, 2 * width), bf16),
            pltpu.VMEM((positions, modes, 2, 2, tile, width), f32),
            pltpu.VMEM((modes, 2 * width, width), bf16),
            pltpu.VMEM((positions, width, width), f32),
            pltpu.VMEM((max(peers - 1, 1), positions, width, width), f32),
            dma((modes,)),
            dma((max(peers - 1, 1), positions, 2)),
            dma((max(peers - 1, 1), positions, 2)),
            pltpu.VMEM((1, width, width), f32),
            pltpu.VMEM((1, width // shape[2], width), f32),
            pltpu.VMEM((8, lanes), f32),
            pltpu.VMEM((count, 8, lanes), f32),
            *[pltpu.VMEM((n + 1, 1, rows, width), f32) for n, rows in sizes],
            *[dma((n,)) for n, _ in sizes],
            *[dma((n + 1,)) for n, _ in sizes],
            dma((1,)),
            dma((1,)),
            dma((count,)),
            dma((count,)),
        ],
        compiler_params=pltpu.CompilerParams(collective_id=1, has_side_effects=True, vmem_limit_bytes=FRONT_LIMIT),
        cost_estimate=pl.CostEstimate(flops=flops, bytes_accessed=0, transcendentals=0),
        name="front",
    )(base, probe, patches, amplitude)


def split_lines(count):
    cores = 2 if count % 2 == 0 else 1
    chips = count // cores
    inner = 1
    while inner * inner * 4 <= chips and chips % (inner * 2) == 0:
        inner *= 2
    return chips // inner, inner, cores


class Shares:
    def __init__(self, spot, width):
        outer, inner, cores = spot.sizes
        self.part = width // cores
        self.own = self.part // (outer * inner)
        self.base = spot.core * self.part
        self.big = (self.part // inner, self.part // outer)
        first = Line(spot, "inner", inner, spot.inner)
        second = Line(spot, "outer", outer, spot.outer)
        self.lines = ((first, second), (second, first))
        self.group = (spot.inner * self.big[0], spot.outer * self.big[1])
        self.offset = (self.group[0] + spot.outer * self.own, self.group[1] + spot.inner * self.own)

    def scatter_parts(self, path, held, sems):
        top = lambda k: rows_at(held, k * self.big[path], self.big[path])
        low = lambda k: rows_at(held, self.group[path] + k * self.own, self.own)
        return [(line, chunk) + pair for line, chunk, pair in zip(self.lines[path], (top, low), sems)]

    def gather_parts(self, path, whole_ref, sems):
        low = lambda k: rows_at(whole_ref, self.base + self.group[path] + k * self.own, self.own)
        top = lambda k: rows_at(whole_ref, self.base + k * self.big[path], self.big[path])
        return [(line, chunk) + pair for line, chunk, pair in zip(self.lines[path][::-1], (low, top), sems)]


def rows_at(ref, start, count):
    return ref.at[:, pl.ds(pl.multiple_of(start, 8), count), :]


def scatter_sizes(shape, width):
    outer, inner, cores = shape
    part = width // cores
    own = part // (outer * inner)
    return [(inner, part // inner), (outer, own), (outer, part // outer), (inner, own)]


def add_rows(into, mine, start, count):
    step = 32 if count % 32 == 0 else count

    def add(i, carry):
        rows = pl.ds(pl.multiple_of(i * step, 8), step)
        into[:, rows, :] += mine[:, pl.ds(pl.multiple_of(start + i * step, 8), step), :]
        return carry

    lax.fori_loop(0, count // step, add, 0)


def broadcast(spot, src, dst, send, recv):
    copies = []
    for step in range(1, spot.count):
        to = lax.rem(spot.me + step, spot.count)
        copies.append(remote(src, dst.at[step], send.at[step], recv.at[step], {"grp": to}))
    return copies


def per_path(spot, count, act):
    for path in range(count):
        @pl.when(spot.core == path)
        def _():
            act(path)


def reduce_kernel(
    shape, modes, width, grad_ref, light_ref, total_ref, dir_ref, pre_ref, sums_ref,
    held, prev, sums_in, sums_all, *rest,
):
    outer, inner, cores = shape
    spot = Spot(outer, inner, cores)
    share = Shares(spot, width)
    slots, (core_s, core_r), sc_s, sc_r, ga_s, ga_r, (back_s, back_r, dir_sem, bc_s, bc_r) = (
        rest[0:4], rest[4:6], rest[6:10], rest[10:14], rest[14:18], rest[18:22], rest[22:]
    )
    pixels = float(width * width)

    barrier = pltpu.get_barrier_semaphore()
    for step in range(1, spot.count):
        to = lax.rem(spot.me + step, spot.count)
        pl.semaphore_signal(barrier, inc=1, device_id={"grp": to}, device_id_type=MESH)

    def load(path, m):
        start = pl.multiple_of(share.base + share.offset[path], 8)
        return pltpu.make_async_copy(dir_ref.at[:, m, pl.ds(start, share.own), :], prev.at[m], dir_sem.at[m])

    def fetch(path):
        for m in range(modes):
            load(path, m).start()

    per_path(spot, cores, fetch)
    sums_in[...] = jnp.zeros_like(sums_in)
    pl.semaphore_wait(barrier, spot.count - 1)

    def give(m):
        other = (1 - spot.core) * share.part
        return remote(
            rows_at(grad_ref.at[m], other, share.part), held.at[m], core_s.at[m], core_r.at[m], spot.partner()
        )

    for m in range(modes):
        give(m).start()
    shift = jnp.sum(total_ref[...]) / pixels

    def scatter_parts(m, path):
        sems = [(slots[k].at[m], sc_s[k].at[m], sc_r[k].at[m]) for k in (2 * path, 2 * path + 1)]
        return share.scatter_parts(path, held.at[m], sems)

    def gather_parts(m, path):
        sems = [(ga_s[k].at[m], ga_r[k].at[m]) for k in (2 * path, 2 * path + 1)]
        return share.gather_parts(path, pre_ref.at[m], sems)

    def home(m):
        block = rows_at(pre_ref.at[m], share.base, share.part)
        return remote(block, block, back_s.at[m], back_r.at[m], spot.partner())

    def stream(m, path):
        give(m).wait_recv()
        add_rows(held.at[m], grad_ref.at[m], share.base, share.part)
        for line, chunk, slot, send, recv in scatter_parts(m, path):
            yield from line.scatter(chunk, slot, send, recv)
        rows = pl.ds(pl.multiple_of(share.offset[path], 8), share.own)
        to = pl.ds(pl.multiple_of(share.base + share.offset[path], 8), share.own)
        light = light_ref[0]
        load(path, m).wait()
        g_re, g_im = held[m, 0, rows, :], held[m, 1, rows, :]
        d_re, d_im = prev[m, 0], prev[m, 1]
        den = light + shift
        p_re, p_im = g_re / den, g_im / den
        pre_ref[m, 0, to, :] = p_re
        pre_ref[m, 1, to, :] = p_im
        (line, chunk, send, recv), later = gather_parts(m, path)
        walk = line.gather(chunk, send, recv)
        next(walk, None)
        terms = (
            g_re * p_re + g_im * p_im,
            g_re * d_re + g_im * d_im,
            light * (p_re * p_re + p_im * p_im),
            light * (p_re * d_re + p_im * d_im),
            light * (d_re * d_re + d_im * d_im),
        )
        for k, term in enumerate(terms):
            row = 5 * m + k
            sums_in[row : row + 1, :] = jnp.sum(fold_lanes(term), axis=0, keepdims=True)
        if m == modes - 1:
            told.append(True)
        yield
        yield from walk
        line, chunk, send, recv = later
        yield from line.gather(chunk, send, recv)
        home(m).start()

    told = []

    def share_sums():
        for copy in broadcast(spot, sums_in, sums_all, bc_s, bc_r):
            copy.start()

    def run(path):
        told.clear()
        streams = [stream(m, path) for m in range(modes)]
        done = set()
        for m in turns(shape, modes, path):
            if m in done:
                continue
            if next(streams[m], done) is done:
                done.add(m)
        share_sums()
        sums_all[0] = sums_in[...]
        for copy in broadcast(spot, sums_in, sums_all, bc_s, bc_r):
            copy.wait_recv()
        for m in range(modes):
            home(m).wait_recv()
        for m in range(modes):
            give(m).wait_send()
            for line, chunk, slot, send, recv in scatter_parts(m, path):
                line.scatter_end(chunk, slot, send, recv)
            for line, chunk, send, recv in gather_parts(m, path):
                line.gather_end(chunk, send, recv)
            home(m).wait_send()
        for copy in broadcast(spot, sums_in, sums_all, bc_s, bc_r):
            copy.wait_send()

    per_path(spot, cores, run)
    sums_ref[...] = jnp.sum(sums_all[...], axis=0)


def turns(shape, modes, path):
    key = (*shape, modes)
    if key in ORDERS:
        return ORDERS[key][path]
    steps = 8 * (shape[0] + shape[1])
    events = sorted((k + (3 * m) // 2, m) for m in range(modes) for k in range(steps))
    return [m for _, m in events]


def reduce_grads(part, light, total, direction):
    modes, _, width, _ = part.shape
    shape = split_lines(lax.axis_size("grp"))
    outer, inner, cores = shape
    count = outer * inner * cores
    sizes = scatter_sizes(shape, width)
    own = sizes[1][1]
    back_sizes = [outer, inner, inner, outer]
    sum_rows = -(-5 * modes // 8) * 8
    lanes = min(128, width)
    dma = pltpu.SemaphoreType.DMA
    f32 = jnp.float32
    scratch = [
        pltpu.VMEM((modes, 2, width // cores, width), f32),
        pltpu.VMEM((modes, 2, own, width), f32),
        pltpu.VMEM((sum_rows, lanes), f32),
        pltpu.VMEM((count, sum_rows, lanes), f32),
    ]
    scratch += [pltpu.VMEM((modes, n + 1, 2, rows, width), f32) for n, rows in sizes]
    scratch += [dma((modes,)), dma((modes,))]
    scratch += [dma((modes, n)) for n, _ in sizes] + [dma((modes, n + 1)) for n, _ in sizes]
    scratch += [dma((modes, 2, n)) for n in back_sizes] + [dma((modes, n)) for n in back_sizes]
    scratch += [dma((modes,)), dma((modes,)), dma((modes,)), dma((count,)), dma((count,))]
    vmem = pl.BlockSpec(memory_space=pltpu.VMEM)
    return pl.pallas_call(
        functools.partial(reduce_kernel, shape, modes, width),
        in_specs=[vmem, vmem, vmem, pl.BlockSpec(memory_space=pl.ANY)],
        out_specs=[vmem, vmem],
        out_shape=[
            jax.ShapeDtypeStruct(part.shape, f32),
            jax.ShapeDtypeStruct((sum_rows, lanes), f32),
        ],
        scratch_shapes=scratch,
        compiler_params=pltpu.CompilerParams(collective_id=0, has_side_effects=True, vmem_limit_bytes=REDUCE_LIMIT),
        cost_estimate=pl.CostEstimate(flops=10**10, bytes_accessed=0, transcendentals=0),
        name="reduce",
    )(part, light, total, direction)


def finish_kernel(norm_ref, sums_ref, pre_ref, probe_ref, dir_ref, new_probe, new_dir, new_norm, kept):
    mode = pl.program_id(0)
    pixels = float(new_probe.shape[3] ** 2)

    @pl.when(pl.program_id(1) == 0)
    def _():
        index = lax.broadcasted_iota(jnp.int32, sums_ref.shape, 0)

        def mean(k):
            return jnp.sum(jnp.where(index == 5 * mode + k, sums_ref[...], 0.0)) / pixels

        norm, cross, light, light_cross, light_prev = (mean(k) for k in range(5))
        new_norm[mode] = norm
        beta = norm / norm_ref[mode]
        upper = norm + beta * cross
        lower = light + beta * (2.0 * light_cross + beta * light_prev)
        kept[0] = beta
        kept[1] = upper / (lower + 1.0)

    beta, alpha = kept[0], kept[1]
    rows = new_probe.shape[2]
    small = min(32, rows)

    def body(i, carry):
        at = pl.ds(pl.multiple_of(i * small, small), small)
        for part in range(2):
            step = pre_ref[0, part, at, :] + beta * dir_ref[part, 0, at, :]
            new_dir[part, 0, at, :] = step
            new_probe[part, 0, at, :] = probe_ref[part, 0, at, :] + alpha * step
        return carry

    lax.fori_loop(0, rows // small, body, 0)


def finish(prev_norm, sums, pre, probe, direction):
    modes, width = probe.shape[1], probe.shape[2]
    rows = min(256, width)
    block = pl.BlockSpec((2, 1, rows, width), lambda m, r: (0, m, r, 0))
    smem = pl.BlockSpec(memory_space=pltpu.SMEM)
    return pl.pallas_call(
        finish_kernel,
        grid=(modes, width // rows),
        in_specs=[
            smem,
            whole(sums.shape),
            pl.BlockSpec((1, 2, rows, width), lambda m, r: (m, 0, r, 0)),
            block,
            block,
        ],
        out_specs=[block, block, smem],
        out_shape=[
            jax.ShapeDtypeStruct(probe.shape, jnp.float32),
            jax.ShapeDtypeStruct(probe.shape, jnp.float32),
            jax.ShapeDtypeStruct((modes,), jnp.float32),
        ],
        scratch_shapes=[pltpu.SMEM((2,), jnp.float32)],
        compiler_params=pltpu.CompilerParams(
            dimension_semantics=("arbitrary", "arbitrary"), vmem_limit_bytes=FINISH_LIMIT
        ),
        name="finish",
    )(prev_norm, sums, pre, probe, direction)


def whole(shape):
    return pl.BlockSpec(shape, lambda *_: (0,) * len(shape))


def on_device(probe, prev_direction, prev_norm, object_tile, offsets, amplitude):
    width = probe.shape[2]
    positions = amplitude.shape[0]
    zero = jnp.int32(0)
    patches = jnp.stack(
        [
            lax.dynamic_slice(object_tile, (zero, offsets[k, 0], offsets[k, 1]), (2, width, width))
            for k in range(positions)
        ]
    )
    part, light, total = front(base_table(width), probe, patches, amplitude)
    pre, sums = reduce_grads(part, light, total, prev_direction)
    return tuple(finish(prev_norm, sums, pre, probe, prev_direction))


def solution(mesh):
    return jax.shard_map(
        on_device,
        mesh=mesh,
        in_specs=(
            P(None, "mode", None, None),
            P(None, "mode", None, None),
            P("mode"),
            P(None, "grp", None),
            P("grp", None),
            P("grp", None, None),
        ),
        out_specs=(P(None, "mode", None, None), P(None, "mode", None, None), P("mode")),
        check_vma=False,
    )
```

```python
import functools
import math

import jax
import numpy as np
import jax.numpy as jnp
from jax import lax
from jax.experimental import pallas as pl
from jax.experimental.pallas import tpu as pltpu
from jax.sharding import PartitionSpec as P

MESH = pl.DeviceIdType.MESH
VMEM_LIMIT = 60 * 1024 * 1024
FRONT_LIMIT = 67043328
REDUCE_LIMIT = 33 * 1024 * 1024
CUT_LIMIT = 16 * 1024 * 1024
FINISH_LIMIT = 18 * 1024 * 1024
ORDERS = {
    (4, 2, 2, 4): (
        (
            0, 1, 3, 0, 1, 0, 1, 1, 0, 2, 1, 0, 0, 0, 3, 1, 1, 2, 1, 0, 2, 3, 1, 1, 1, 3, 0, 0, 2,
            2, 1, 2, 3, 1, 2, 0, 3, 2, 0, 0, 3, 3, 1, 0, 2, 2, 2, 1, 2, 2, 3, 3, 2, 3, 3, 3, 3, 0,
            2, 3,
        ),
        (
            0, 1, 0, 0, 1, 0, 3, 2, 0, 1, 0, 2, 0, 3, 1, 2, 1, 1, 0, 1, 0, 2, 2, 0, 1, 0, 3, 3, 3,
            1, 2, 2, 0, 3, 0, 2, 0, 2, 1, 3, 2, 1, 3, 1, 2, 3, 2, 3, 1, 1, 1, 2, 2, 2, 3, 3, 0, 3,
            3, 3,
        ),
    ),
}


def base_table(width):
    index = np.arange(width, dtype=np.int64)
    product = index[:, None] * index[None, :] % width
    angle = np.float32(-2.0 * math.pi / width) * product.astype(np.float32)
    scale = np.float32(1.0 / math.sqrt(width))
    both = np.stack([np.cos(angle) * scale, np.sin(angle) * scale])
    return jnp.asarray(both.astype(jnp.bfloat16))


def fold_lanes(block):
    rows, width = block.shape
    lanes = min(128, width)
    acc = jnp.sum(block.reshape(rows // 8, 8, width), axis=0)
    out = acc[:, :lanes]
    for at in range(lanes, width, lanes):
        out = out + acc[:, at : at + lanes]
    return out


class Spot:
    def __init__(self, outer, inner, cores):
        me = lax.axis_index("grp")
        self.me = me
        self.sizes = (outer, inner, cores)
        self.count = outer * inner * cores
        self.core = lax.rem(me, cores)
        self.inner = lax.rem(me // cores, inner)
        self.outer = me // (cores * inner)
        self.stride = {"core": 1, "inner": cores, "outer": cores * inner}

    def at(self, line, step):
        return {"grp": self.me + step * self.stride[line]}

    def partner(self):
        return {"grp": self.me + 1 - 2 * self.core}


def remote(src, dst, send, recv, device):
    return pltpu.make_async_remote_copy(
        src_ref=src, dst_ref=dst, send_sem=send, recv_sem=recv, device_id=device, device_id_type=MESH
    )


class Line:
    def __init__(self, spot, name, length, place):
        self.spot, self.name, self.length, self.place = spot, name, length, place

    def scatter(self, chunk, slots, send, recv):
        size, u = self.length, self.place

        def take(slot, into):
            got = remote(slots.at[slot], slots.at[slot], send.at[0], recv.at[slot], self.spot.at(self.name, 0))
            got.wait_recv()
            into[...] += slots[slot]

        def push(k, step, slot):
            remote(chunk(k), slots.at[slot], send.at[k], recv.at[slot], self.spot.at(self.name, step)).start()

        for step in range(size - 1):
            right, left = size - 1 - step, step

            @pl.when(u < right)
            def _():
                @pl.when(u > 0)
                def _():
                    take(right + 1, chunk(right))

                push(right, 1, right + 1)

            if size > 2:
                yield

            @pl.when(u > left)
            def _():
                @pl.when(u < size - 1)
                def _():
                    take(left, chunk(left))

                push(left, -1, left)

            yield

        @pl.when(u > 0)
        def _():
            take(u + 1, chunk(u))

        @pl.when(u < size - 1)
        def _():
            take(u, chunk(u))

    def scatter_end(self, chunk, slots, send, recv):
        for k in range(self.length):
            @pl.when(self.place != k)
            def _():
                remote(chunk(k), slots.at[0], send.at[k], recv.at[0], self.spot.at(self.name, 0)).wait_send()

    def gather(self, chunk, send, recv):
        size, u = self.length, self.place

        def push(k, way, step):
            remote(chunk(k), chunk(k), send.at[way, k], recv.at[k], self.spot.at(self.name, step)).start()

        def take(k):
            remote(chunk(k), chunk(k), send.at[0, 0], recv.at[k], self.spot.at(self.name, 0)).wait_recv()

        for step in range(size):
            low, high = u - step, u + step

            @pl.when(low >= 0)
            def _():
                if step > 0:
                    take(low)

                @pl.when(u < size - 1)
                def _():
                    push(low, 0, 1)

            if size > 2 and step > 0:
                yield

            @pl.when(high < size)
            def _():
                if step > 0:
                    take(high)

                @pl.when(u > 0)
                def _():
                    push(high, 1, -1)

            if step < size - 1:
                yield

    def gather_end(self, chunk, send, recv):
        size, u = self.length, self.place
        for k in range(size):
            for way in range(2):
                @pl.when((u < size - 1) & (u >= k) if way == 0 else (u > 0) & (u <= k))
                def _():
                    remote(chunk(k), chunk(k), send.at[way, k], recv.at[k], self.spot.at(self.name, 0)).wait_send()


def build_tables(base_ref, plus, minus):
    width = base_ref.shape[1]
    tile = width // 2
    for row in range(2):
        for col in range(2):
            take = (pl.ds(row * tile, tile), pl.ds(col * tile, tile))
            cosine, sine = base_ref[(0, *take)], base_ref[(1, *take)]
            for ref, upper, lower in ((plus, sine, -sine), (minus, -sine, sine)):
                r, c = row * width, col * width
                ref[r : r + tile, c : c + tile] = cosine
                ref[r + tile : r + width, c + tile : c + width] = cosine
                ref[r : r + tile, c + tile : c + width] = upper
                ref[r + tile : r + width, c : c + tile] = lower


def front_kernel(
    peers, shape, base_ref, probe_ref, patch_ref, amp_ref, grad_ref, light_ref, total_ref,
    plus, minus, probe, exits, wave, stacked, own, other, load_sem, send_sem, recv_sem,
    lit, held, tile_in, tile_all, *rest,
):
    slots, sc_s, sc_r, (core_s, core_r, bc_s, bc_r) = rest[0:4], rest[4:8], rest[8:12], rest[12:]
    spot = Spot(*shape)
    positions, modes = exits.shape[0], exits.shape[1]
    width = base_ref.shape[1]
    tile = width // 2
    step = min(64, tile)
    f32, bf16 = jnp.float32, jnp.bfloat16
    y = lax.axis_index("mode")

    barrier = pltpu.get_barrier_semaphore()
    for k in range(1, peers):
        pl.semaphore_signal(barrier, inc=1, device_id={"mode": lax.rem(y + k, peers)}, device_id_type=MESH)
    for k in range(1, spot.count):
        to = lax.rem(spot.me + k, spot.count)
        pl.semaphore_signal(barrier, inc=1, device_id={"grp": to}, device_id_type=MESH)

    def load(m):
        return pltpu.make_async_copy(probe_ref.at[:, m], probe.at[m], load_sem.at[m])

    for m in range(modes):
        load(m).start()
    build_tables(base_ref, plus, minus)
    share = Shares(spot, width)
    pl.semaphore_wait(barrier, peers - 1 + spot.count - 1)

    def swap(p, t, k):
        rows = pl.ds(t * tile, tile)
        return remote(
            own.at[p, rows], other.at[k - 1, p, rows], send_sem.at[k - 1, p, t], recv_sem.at[k - 1, p, t],
            {"mode": lax.rem(y + k, peers)},
        )

    def put(half, m, rows):
        for col in range(2):
            for part in range(2):
                block = half[:, (2 * col + part) * tile : (2 * col + part + 1) * tile]
                stacked[m, pl.ds(rows * width + part * tile, tile), col * tile : (col + 1) * tile] = block

    def leave(p, m):
        def body(i, carry):
            rows = pl.ds(pl.multiple_of(i * step, step), step)
            for col in range(2):
                at = pl.ds(col * tile, tile)
                obj_re = patch_ref[p, 0, rows, at].astype(f32)
                obj_im = patch_ref[p, 1, rows, at].astype(f32)
                pro_re, pro_im = probe[m, 0, rows, at], probe[m, 1, rows, at]
                exits[p, m, rows, 2 * col * tile : (2 * col + 1) * tile] = (pro_re * obj_re - pro_im * obj_im).astype(bf16)
                exits[p, m, rows, (2 * col + 1) * tile : (2 * col + 2) * tile] = (pro_re * obj_im + pro_im * obj_re).astype(bf16)
            return carry

        lax.fori_loop(0, width // step, body, 0)

    def forward(p, carry):
        def first(m, carry):
            @pl.when(p == 0)
            def _():
                load(m).wait()

            leave(p, m)
            half = jnp.dot(exits[p, m], plus[...], preferred_element_type=f32).astype(bf16)
            for rows in range(2):
                put(half[rows * tile : (rows + 1) * tile], m, rows)
            return carry

        lax.fori_loop(0, modes, first, 0)
        for t in range(2):
            rows = pl.ds(t * tile, tile)

            def second(m, carry):
                out = jnp.dot(minus[t * width : (t + 1) * width, :], stacked[m], preferred_element_type=f32)
                real, imag = out[:tile], out[tile:]
                wave[p, m, t, 0] = real
                wave[p, m, t, 1] = imag
                light = real * real + imag * imag
                own[p, rows, :] = jnp.where(m == 0, light, own[p, rows, :] + light)
                return carry

            lax.fori_loop(0, modes, second, 0)
            for k in range(1, peers):
                swap(p, t, k).start()
        return carry

    lax.fori_loop(0, positions, forward, 0)

    def give():
        away = rows_at(lit, (1 - spot.core) * share.part, share.part)
        return remote(away, held, core_s.at[0], core_r.at[0], spot.partner())

    def shine(i, carry):
        rows = pl.ds(pl.multiple_of(i * step, step), step)
        acc = jnp.zeros((step, width), f32)
        for p in range(positions):
            obj_re, obj_im = patch_ref[p, 0, rows, :].astype(f32), patch_ref[p, 1, rows, :].astype(f32)
            acc = acc + obj_re * obj_re + obj_im * obj_im
        lit[0, rows, :] = acc
        return carry

    def parts(path):
        sems = [(slots[k], sc_s[k], sc_r[k]) for k in (2 * path, 2 * path + 1)]
        return share.scatter_parts(path, held, sems)

    def scatter(path):
        for line, chunk, slot, send, recv in parts(path):
            for _ in line.scatter(chunk, slot, send, recv):
                pass
        block = held[0, pl.ds(pl.multiple_of(share.offset[path], 8), share.own), :]
        light_ref[0] = block
        tile_in[...] = fold_lanes(block)

    def scatter_end(path):
        for line, chunk, slot, send, recv in parts(path):
            line.scatter_end(chunk, slot, send, recv)

    lax.fori_loop(0, width // step, shine, 0)
    give().start()
    give().wait_recv()
    add_rows(held, lit, share.base, share.part)
    per_path(spot, shape[2], scatter)
    for copy in broadcast(spot, tile_in, tile_all, bc_s, bc_r):
        copy.start()
    tile_all[0] = tile_in[...]

    def backward(p, carry):
        for t in range(2):
            for k in range(1, peers):
                swap(p, t, k).wait_recv()

            def scale(i, carry):
                rows = pl.ds(pl.multiple_of(t * tile + i * step, step), step)
                total = own[p, rows, :]
                for k in range(peers - 1):
                    total = total + other[k, p, rows, :]
                ratio = amp_ref[p, rows, :].astype(f32) / jnp.sqrt(total + 1.0)
                here = pl.ds(pl.multiple_of(i * step, step), step)

                def fix(m, carry):
                    for part in range(2):
                        wave[p, m, t, part, here, :] = wave[p, m, t, part, here, :] * ratio
                    return carry

                lax.fori_loop(0, modes, fix, 0)
                return carry

            lax.fori_loop(0, tile // step, scale, 0)

            def first(m, carry):
                fixed = [wave[p, m, t, part].astype(bf16) for part in range(2)]
                blocks = [fixed[part][:, col * tile : (col + 1) * tile] for col in range(2) for part in range(2)]
                joined = jnp.concatenate(blocks, axis=1)
                half = jnp.dot(joined, minus[...], preferred_element_type=f32).astype(bf16)
                put(half, m, t)
                return carry

            lax.fori_loop(0, modes, first, 0)

        def second(m, carry):
            for t in range(2):
                rows = pl.ds(t * tile, tile)
                out = jnp.dot(plus[t * width : (t + 1) * width, :], stacked[m], preferred_element_type=f32)
                for col in range(2):
                    at = pl.ds(col * tile, tile)
                    real, imag = out[:tile, col * tile : (col + 1) * tile], out[tile:, col * tile : (col + 1) * tile]
                    obj_re = patch_ref[p, 0, rows, at].astype(f32)
                    obj_im = patch_ref[p, 1, rows, at].astype(f32)
                    diff_re = real - exits[p, m, rows, 2 * col * tile : (2 * col + 1) * tile].astype(f32)
                    diff_im = imag - exits[p, m, rows, (2 * col + 1) * tile : (2 * col + 2) * tile].astype(f32)
                    add_re = obj_re * diff_re + obj_im * diff_im
                    add_im = obj_re * diff_im - obj_im * diff_re
                    grad_ref[m, 0, rows, at] = jnp.where(p == 0, add_re, grad_ref[m, 0, rows, at] + add_re)
                    grad_ref[m, 1, rows, at] = jnp.where(p == 0, add_im, grad_ref[m, 1, rows, at] + add_im)
            return carry

        lax.fori_loop(0, modes, second, 0)
        return carry

    lax.fori_loop(0, positions, backward, 0)
    for copy in broadcast(spot, tile_in, tile_all, bc_s, bc_r):
        copy.wait()
    total_ref[...] = jnp.sum(tile_all[...], axis=0)
    give().wait_send()
    per_path(spot, shape[2], scatter_end)
    for p in range(positions):
        for t in range(2):
            for k in range(1, peers):
                swap(p, t, k).wait_send()


def front(base, probe, patches, amplitude):
    modes, width = probe.shape[1], probe.shape[2]
    positions = patches.shape[0]
    peers = lax.axis_size("mode")
    tile = width // 2
    dma = pltpu.SemaphoreType.DMA
    f32, bf16 = jnp.float32, jnp.bfloat16
    vmem = pl.BlockSpec(memory_space=pltpu.VMEM)
    shape = split_lines(lax.axis_size("grp"))
    sizes = scatter_sizes(shape, width)
    count, lanes = lax.axis_size("grp"), min(128, width)
    flops = positions * modes * 2 * 16 * width**3
    return pl.pallas_call(
        functools.partial(front_kernel, peers, shape),
        in_specs=[vmem, pl.BlockSpec(memory_space=pl.ANY), vmem, vmem],
        out_specs=[vmem, vmem, vmem],
        out_shape=[
            jax.ShapeDtypeStruct((modes, 2, width, width), f32),
            jax.ShapeDtypeStruct((1, sizes[1][1], width), f32),
            jax.ShapeDtypeStruct((8, lanes), f32),
        ],
        scratch_shapes=[
            pltpu.VMEM((2 * width, 2 * width), bf16),
            pltpu.VMEM((2 * width, 2 * width), bf16),
            pltpu.VMEM((modes, 2, width, width), f32),
            pltpu.VMEM((positions, modes, width, 2 * width), bf16),
            pltpu.VMEM((positions, modes, 2, 2, tile, width), f32),
            pltpu.VMEM((modes, 2 * width, width), bf16),
            pltpu.VMEM((positions, width, width), f32),
            pltpu.VMEM((max(peers - 1, 1), positions, width, width), f32),
            dma((modes,)),
            dma((max(peers - 1, 1), positions, 2)),
            dma((max(peers - 1, 1), positions, 2)),
            pltpu.VMEM((1, width, width), f32),
            pltpu.VMEM((1, width // shape[2], width), f32),
            pltpu.VMEM((8, lanes), f32),
            pltpu.VMEM((count, 8, lanes), f32),
            *[pltpu.VMEM((n + 1, 1, rows, width), f32) for n, rows in sizes],
            *[dma((n,)) for n, _ in sizes],
            *[dma((n + 1,)) for n, _ in sizes],
            dma((1,)),
            dma((1,)),
            dma((count,)),
            dma((count,)),
        ],
        compiler_params=pltpu.CompilerParams(collective_id=1, has_side_effects=True, vmem_limit_bytes=FRONT_LIMIT),
        cost_estimate=pl.CostEstimate(flops=flops, bytes_accessed=0, transcendentals=0),
        name="front",
    )(base, probe, patches, amplitude)


def split_lines(count):
    cores = 2 if count % 2 == 0 else 1
    chips = count // cores
    inner = 1
    while inner * inner * 4 <= chips and chips % (inner * 2) == 0:
        inner *= 2
    return chips // inner, inner, cores


class Shares:
    def __init__(self, spot, width):
        outer, inner, cores = spot.sizes
        self.part = width // cores
        self.own = self.part // (outer * inner)
        self.base = spot.core * self.part
        self.big = (self.part // inner, self.part // outer)
        first = Line(spot, "inner", inner, spot.inner)
        second = Line(spot, "outer", outer, spot.outer)
        self.lines = ((first, second), (second, first))
        self.group = (spot.inner * self.big[0], spot.outer * self.big[1])
        self.offset = (self.group[0] + spot.outer * self.own, self.group[1] + spot.inner * self.own)

    def scatter_parts(self, path, held, sems):
        top = lambda k: rows_at(held, k * self.big[path], self.big[path])
        low = lambda k: rows_at(held, self.group[path] + k * self.own, self.own)
        return [(line, chunk) + pair for line, chunk, pair in zip(self.lines[path], (top, low), sems)]

    def gather_parts(self, path, whole_ref, sems):
        low = lambda k: rows_at(whole_ref, self.base + self.group[path] + k * self.own, self.own)
        top = lambda k: rows_at(whole_ref, self.base + k * self.big[path], self.big[path])
        return [(line, chunk) + pair for line, chunk, pair in zip(self.lines[path][::-1], (low, top), sems)]


def rows_at(ref, start, count):
    return ref.at[:, pl.ds(pl.multiple_of(start, 8), count), :]


def scatter_sizes(shape, width):
    outer, inner, cores = shape
    part = width // cores
    own = part // (outer * inner)
    return [(inner, part // inner), (outer, own), (outer, part // outer), (inner, own)]


def add_rows(into, mine, start, count):
    step = 32 if count % 32 == 0 else count

    def add(i, carry):
        rows = pl.ds(pl.multiple_of(i * step, 8), step)
        into[:, rows, :] += mine[:, pl.ds(pl.multiple_of(start + i * step, 8), step), :]
        return carry

    lax.fori_loop(0, count // step, add, 0)


def broadcast(spot, src, dst, send, recv):
    copies = []
    for step in range(1, spot.count):
        to = lax.rem(spot.me + step, spot.count)
        copies.append(remote(src, dst.at[step], send.at[step], recv.at[step], {"grp": to}))
    return copies


def per_path(spot, count, act):
    for path in range(count):
        @pl.when(spot.core == path)
        def _():
            act(path)


def reduce_kernel(
    shape, modes, width, grad_ref, light_ref, total_ref, dir_ref, pre_ref, sums_ref,
    held, prev, sums_in, sums_all, *rest,
):
    outer, inner, cores = shape
    spot = Spot(outer, inner, cores)
    share = Shares(spot, width)
    slots, (core_s, core_r), sc_s, sc_r, ga_s, ga_r, (back_s, back_r, dir_sem, bc_s, bc_r) = (
        rest[0:4], rest[4:6], rest[6:10], rest[10:14], rest[14:18], rest[18:22], rest[22:]
    )
    pixels = float(width * width)

    barrier = pltpu.get_barrier_semaphore()
    for step in range(1, spot.count):
        to = lax.rem(spot.me + step, spot.count)
        pl.semaphore_signal(barrier, inc=1, device_id={"grp": to}, device_id_type=MESH)

    def load(path, m):
        start = pl.multiple_of(share.base + share.offset[path], 8)
        return pltpu.make_async_copy(dir_ref.at[:, m, pl.ds(start, share.own), :], prev.at[m], dir_sem.at[m])

    def fetch(path):
        for m in range(modes):
            load(path, m).start()

    per_path(spot, cores, fetch)
    sums_in[...] = jnp.zeros_like(sums_in)
    pl.semaphore_wait(barrier, spot.count - 1)

    def give(m):
        other = (1 - spot.core) * share.part
        return remote(
            rows_at(grad_ref.at[m], other, share.part), held.at[m], core_s.at[m], core_r.at[m], spot.partner()
        )

    for m in range(modes):
        give(m).start()
    shift = jnp.sum(total_ref[...]) / pixels

    def scatter_parts(m, path):
        sems = [(slots[k].at[m], sc_s[k].at[m], sc_r[k].at[m]) for k in (2 * path, 2 * path + 1)]
        return share.scatter_parts(path, held.at[m], sems)

    def gather_parts(m, path):
        sems = [(ga_s[k].at[m], ga_r[k].at[m]) for k in (2 * path, 2 * path + 1)]
        return share.gather_parts(path, pre_ref.at[m], sems)

    def home(m):
        block = rows_at(pre_ref.at[m], share.base, share.part)
        return remote(block, block, back_s.at[m], back_r.at[m], spot.partner())

    def stream(m, path):
        give(m).wait_recv()
        add_rows(held.at[m], grad_ref.at[m], share.base, share.part)
        for line, chunk, slot, send, recv in scatter_parts(m, path):
            yield from line.scatter(chunk, slot, send, recv)
        rows = pl.ds(pl.multiple_of(share.offset[path], 8), share.own)
        to = pl.ds(pl.multiple_of(share.base + share.offset[path], 8), share.own)
        light = light_ref[0]
        load(path, m).wait()
        g_re, g_im = held[m, 0, rows, :], held[m, 1, rows, :]
        d_re, d_im = prev[m, 0], prev[m, 1]
        den = light + shift
        p_re, p_im = g_re / den, g_im / den
        pre_ref[m, 0, to, :] = p_re
        pre_ref[m, 1, to, :] = p_im
        (line, chunk, send, recv), later = gather_parts(m, path)
        walk = line.gather(chunk, send, recv)
        next(walk, None)
        terms = (
            g_re * p_re + g_im * p_im,
            g_re * d_re + g_im * d_im,
            light * (p_re * p_re + p_im * p_im),
            light * (p_re * d_re + p_im * d_im),
            light * (d_re * d_re + d_im * d_im),
        )
        for k, term in enumerate(terms):
            row = 5 * m + k
            sums_in[row : row + 1, :] = jnp.sum(fold_lanes(term), axis=0, keepdims=True)
        if m == modes - 1:
            told.append(True)
        yield
        yield from walk
        line, chunk, send, recv = later
        yield from line.gather(chunk, send, recv)
        home(m).start()

    told = []

    def share_sums():
        for copy in broadcast(spot, sums_in, sums_all, bc_s, bc_r):
            copy.start()

    def run(path):
        told.clear()
        streams = [stream(m, path) for m in range(modes)]
        done = set()
        for m in turns(shape, modes, path):
            if m in done:
                continue
            if next(streams[m], done) is done:
                done.add(m)
        share_sums()
        sums_all[0] = sums_in[...]
        for copy in broadcast(spot, sums_in, sums_all, bc_s, bc_r):
            copy.wait_recv()
        for m in range(modes):
            home(m).wait_recv()
        for m in range(modes):
            give(m).wait_send()
            for line, chunk, slot, send, recv in scatter_parts(m, path):
                line.scatter_end(chunk, slot, send, recv)
            for line, chunk, send, recv in gather_parts(m, path):
                line.gather_end(chunk, send, recv)
            home(m).wait_send()
        for copy in broadcast(spot, sums_in, sums_all, bc_s, bc_r):
            copy.wait_send()

    per_path(spot, cores, run)
    sums_ref[...] = jnp.sum(sums_all[...], axis=0)


def turns(shape, modes, path):
    key = (*shape, modes)
    if key in ORDERS:
        return ORDERS[key][path]
    steps = 8 * (shape[0] + shape[1])
    events = sorted((k + (3 * m) // 2, m) for m in range(modes) for k in range(steps))
    return [m for _, m in events]


def reduce_grads(part, light, total, direction):
    modes, _, width, _ = part.shape
    shape = split_lines(lax.axis_size("grp"))
    outer, inner, cores = shape
    count = outer * inner * cores
    sizes = scatter_sizes(shape, width)
    own = sizes[1][1]
    back_sizes = [outer, inner, inner, outer]
    sum_rows = -(-5 * modes // 8) * 8
    lanes = min(128, width)
    dma = pltpu.SemaphoreType.DMA
    f32 = jnp.float32
    scratch = [
        pltpu.VMEM((modes, 2, width // cores, width), f32),
        pltpu.VMEM((modes, 2, own, width), f32),
        pltpu.VMEM((sum_rows, lanes), f32),
        pltpu.VMEM((count, sum_rows, lanes), f32),
    ]
    scratch += [pltpu.VMEM((modes, n + 1, 2, rows, width), f32) for n, rows in sizes]
    scratch += [dma((modes,)), dma((modes,))]
    scratch += [dma((modes, n)) for n, _ in sizes] + [dma((modes, n + 1)) for n, _ in sizes]
    scratch += [dma((modes, 2, n)) for n in back_sizes] + [dma((modes, n)) for n in back_sizes]
    scratch += [dma((modes,)), dma((modes,)), dma((modes,)), dma((count,)), dma((count,))]
    vmem = pl.BlockSpec(memory_space=pltpu.VMEM)
    return pl.pallas_call(
        functools.partial(reduce_kernel, shape, modes, width),
        in_specs=[vmem, vmem, vmem, pl.BlockSpec(memory_space=pl.ANY)],
        out_specs=[vmem, vmem],
        out_shape=[
            jax.ShapeDtypeStruct(part.shape, f32),
            jax.ShapeDtypeStruct((sum_rows, lanes), f32),
        ],
        scratch_shapes=scratch,
        compiler_params=pltpu.CompilerParams(collective_id=0, has_side_effects=True, vmem_limit_bytes=REDUCE_LIMIT),
        cost_estimate=pl.CostEstimate(flops=10**10, bytes_accessed=0, transcendentals=0),
        name="reduce",
    )(part, light, total, direction)


def finish_kernel(norm_ref, sums_ref, pre_ref, probe_ref, dir_ref, new_probe, new_dir, new_norm, kept):
    mode = pl.program_id(0)
    pixels = float(new_probe.shape[3] ** 2)

    @pl.when(pl.program_id(1) == 0)
    def _():
        index = lax.broadcasted_iota(jnp.int32, sums_ref.shape, 0)

        def mean(k):
            return jnp.sum(jnp.where(index == 5 * mode + k, sums_ref[...], 0.0)) / pixels

        norm, cross, light, light_cross, light_prev = (mean(k) for k in range(5))
        new_norm[mode] = norm
        beta = norm / norm_ref[mode]
        upper = norm + beta * cross
        lower = light + beta * (2.0 * light_cross + beta * light_prev)
        kept[0] = beta
        kept[1] = upper / (lower + 1.0)

    beta, alpha = kept[0], kept[1]
    rows = new_probe.shape[2]
    small = min(32, rows)

    def body(i, carry):
        at = pl.ds(pl.multiple_of(i * small, small), small)
        for part in range(2):
            step = pre_ref[0, part, at, :] + beta * dir_ref[part, 0, at, :]
            new_dir[part, 0, at, :] = step
            new_probe[part, 0, at, :] = probe_ref[part, 0, at, :] + alpha * step
        return carry

    lax.fori_loop(0, rows // small, body, 0)


def finish(prev_norm, sums, pre, probe, direction):
    modes, width = probe.shape[1], probe.shape[2]
    rows = min(256, width)
    block = pl.BlockSpec((2, 1, rows, width), lambda m, r: (0, m, r, 0))
    smem = pl.BlockSpec(memory_space=pltpu.SMEM)
    return pl.pallas_call(
        finish_kernel,
        grid=(modes, width // rows),
        in_specs=[
            smem,
            whole(sums.shape),
            pl.BlockSpec((1, 2, rows, width), lambda m, r: (m, 0, r, 0)),
            block,
            block,
        ],
        out_specs=[block, block, smem],
        out_shape=[
            jax.ShapeDtypeStruct(probe.shape, jnp.float32),
            jax.ShapeDtypeStruct(probe.shape, jnp.float32),
            jax.ShapeDtypeStruct((modes,), jnp.float32),
        ],
        scratch_shapes=[pltpu.SMEM((2,), jnp.float32)],
        compiler_params=pltpu.CompilerParams(
            dimension_semantics=("arbitrary", "arbitrary"), vmem_limit_bytes=FINISH_LIMIT
        ),
        name="finish",
    )(prev_norm, sums, pre, probe, direction)


def cut_kernel(offset_ref, tile_ref, patch_ref, wide):
    positions, width, full = patch_ref.shape[0], patch_ref.shape[2], tile_ref.shape[2]
    step = 64 if width % 64 == 0 else width

    def widen(i, carry):
        rows = pl.ds(pl.multiple_of(i * step, step), step)
        for part in range(2):
            wide[part, rows, :] = tile_ref[part, rows, :].astype(jnp.float32)
        return carry

    lax.fori_loop(0, full // step, widen, 0)

    def position(p, carry):
        row, col = offset_ref[p, 0], offset_ref[p, 1]
        turn = lax.rem(full - col, full)
        low = lax.rem(row, 8)
        lift = lax.rem(step + 8 - low, step + 8)

        def body(i, carry):
            for part in range(2):
                block = wide[part, pl.ds(pl.multiple_of(row - low + i * step, 8), step + 8), :]
                block = pltpu.roll(pltpu.roll(block, lift, 0)[:step], turn, 1)[:, :width]
                patch_ref[p, part, pl.ds(pl.multiple_of(i * step, step), step), :] = block.astype(jnp.bfloat16)
            return carry

        lax.fori_loop(0, width // step, body, 0)
        return carry

    lax.fori_loop(0, positions, position, 0)


def cut(offsets, tile, width):
    positions = offsets.shape[0]
    vmem = pl.BlockSpec(memory_space=pltpu.VMEM)
    return pl.pallas_call(
        cut_kernel,
        in_specs=[pl.BlockSpec(memory_space=pltpu.SMEM), vmem],
        out_specs=vmem,
        out_shape=jax.ShapeDtypeStruct((positions, 2, width, width), jnp.bfloat16),
        scratch_shapes=[pltpu.VMEM((2, tile.shape[1] + 8, tile.shape[2]), jnp.float32)],
        compiler_params=pltpu.CompilerParams(vmem_limit_bytes=CUT_LIMIT),
        name="cut",
    )(offsets, tile)


def whole(shape):
    return pl.BlockSpec(shape, lambda *_: (0,) * len(shape))


def on_device(probe, prev_direction, prev_norm, object_tile, offsets, amplitude):
    width = probe.shape[2]
    patches = cut(offsets, object_tile, width)
    part, light, total = front(base_table(width), probe, patches, amplitude)
    pre, sums = reduce_grads(part, light, total, prev_direction)
    return tuple(finish(prev_norm, sums, pre, probe, prev_direction))


def solution(mesh):
    return jax.shard_map(
        on_device,
        mesh=mesh,
        in_specs=(
            P(None, "mode", None, None),
            P(None, "mode", None, None),
            P("mode"),
            P(None, "grp", None),
            P("grp", None),
            P("grp", None, None),
        ),
        out_specs=(P(None, "mode", None, None), P(None, "mode", None, None), P("mode")),
        check_vma=False,
    )
```

```python
import functools
import math

import jax
import numpy as np
import jax.numpy as jnp
from jax import lax
from jax.experimental import pallas as pl
from jax.experimental.pallas import tpu as pltpu
from jax.sharding import PartitionSpec as P

MESH = pl.DeviceIdType.MESH
VMEM_LIMIT = 60 * 1024 * 1024
FRONT_LIMIT = 67043328
CUT_LIMIT = 16 * 1024 * 1024
FINISH_LIMIT = 60 * 1024 * 1024
ORDERS = {
    (4, 2, 2, 4): (
        (
            4, 4, 4, 4, 0, 1, 3, 0, 1, 0, 1, 1, 0, 2, 1, 0, 0, 0, 3, 1, 1, 2, 1, 0, 2, 3, 1, 1, 1,
            3, 0, 0, 2, 2, 1, 2, 3, 1, 2, 0, 3, 2, 0, 0, 3, 3, 1, 0, 2, 2, 2, 1, 2, 2, 3, 3, 2, 3,
            3, 3, 3, 0, 2, 3,
        ),
        (
            4, 4, 4, 4, 0, 1, 0, 0, 1, 0, 3, 2, 0, 1, 0, 2, 0, 3, 1, 2, 1, 1, 0, 1, 0, 2, 2, 0, 1,
            0, 3, 3, 3, 1, 2, 2, 0, 3, 0, 2, 0, 2, 1, 3, 2, 1, 3, 1, 2, 3, 2, 3, 1, 1, 1, 2, 2, 2,
            3, 3, 0, 3, 3, 3,
        ),
    ),
}


def base_table(width):
    index = np.arange(width, dtype=np.int64)
    product = index[:, None] * index[None, :] % width
    angle = np.float32(-2.0 * math.pi / width) * product.astype(np.float32)
    scale = np.float32(1.0 / math.sqrt(width))
    both = np.stack([np.cos(angle) * scale, np.sin(angle) * scale])
    return jnp.asarray(both.astype(jnp.bfloat16))


def fold_lanes(block):
    rows, width = block.shape
    lanes = min(128, width)
    acc = jnp.sum(block.reshape(rows // 8, 8, width), axis=0)
    out = acc[:, :lanes]
    for at in range(lanes, width, lanes):
        out = out + acc[:, at : at + lanes]
    return out


class Spot:
    def __init__(self, outer, inner, cores):
        me = lax.axis_index("grp")
        self.me = me
        self.sizes = (outer, inner, cores)
        self.count = outer * inner * cores
        self.core = lax.rem(me, cores)
        self.inner = lax.rem(me // cores, inner)
        self.outer = me // (cores * inner)
        self.stride = {"core": 1, "inner": cores, "outer": cores * inner}

    def at(self, line, step):
        return {"grp": self.me + step * self.stride[line]}

    def partner(self):
        return {"grp": self.me + 1 - 2 * self.core}


def remote(src, dst, send, recv, device):
    return pltpu.make_async_remote_copy(
        src_ref=src, dst_ref=dst, send_sem=send, recv_sem=recv, device_id=device, device_id_type=MESH
    )


class Line:
    def __init__(self, spot, name, length, place):
        self.spot, self.name, self.length, self.place = spot, name, length, place

    def scatter(self, chunk, slots, send, recv):
        size, u = self.length, self.place

        def take(slot, into):
            got = remote(slots(slot), slots(slot), send.at[0], recv.at[slot], self.spot.at(self.name, 0))
            got.wait_recv()
            into[...] += slots(slot)[...]

        def push(k, step, slot):
            remote(chunk(k), slots(slot), send.at[k], recv.at[slot], self.spot.at(self.name, step)).start()

        for step in range(size - 1):
            right, left = size - 1 - step, step

            @pl.when(u < right)
            def _():
                @pl.when(u > 0)
                def _():
                    take(right + 1, chunk(right))

                push(right, 1, right + 1)

            if size > 2:
                yield

            @pl.when(u > left)
            def _():
                @pl.when(u < size - 1)
                def _():
                    take(left, chunk(left))

                push(left, -1, left)

            yield

        @pl.when(u > 0)
        def _():
            take(u + 1, chunk(u))

        @pl.when(u < size - 1)
        def _():
            take(u, chunk(u))

    def scatter_end(self, chunk, slots, send, recv):
        for k in range(self.length):
            @pl.when(self.place != k)
            def _():
                remote(chunk(k), slots(0), send.at[k], recv.at[0], self.spot.at(self.name, 0)).wait_send()

    def gather(self, chunk, send, recv):
        size, u = self.length, self.place

        def push(k, way, step):
            remote(chunk(k), chunk(k), send.at[way, k], recv.at[k], self.spot.at(self.name, step)).start()

        def take(k):
            remote(chunk(k), chunk(k), send.at[0, 0], recv.at[k], self.spot.at(self.name, 0)).wait_recv()

        for step in range(size):
            low, high = u - step, u + step

            @pl.when(low >= 0)
            def _():
                if step > 0:
                    take(low)

                @pl.when(u < size - 1)
                def _():
                    push(low, 0, 1)

            if size > 2 and step > 0:
                yield

            @pl.when(high < size)
            def _():
                if step > 0:
                    take(high)

                @pl.when(u > 0)
                def _():
                    push(high, 1, -1)

            if step < size - 1:
                yield

    def gather_end(self, chunk, send, recv):
        size, u = self.length, self.place
        for k in range(size):
            for way in range(2):
                @pl.when((u < size - 1) & (u >= k) if way == 0 else (u > 0) & (u <= k))
                def _():
                    remote(chunk(k), chunk(k), send.at[way, k], recv.at[k], self.spot.at(self.name, 0)).wait_send()


def build_tables(base_ref, plus, minus):
    width = base_ref.shape[1]
    tile = width // 2
    for row in range(2):
        for col in range(2):
            take = (pl.ds(row * tile, tile), pl.ds(col * tile, tile))
            cosine, sine = base_ref[(0, *take)], base_ref[(1, *take)]
            for ref, upper, lower in ((plus, sine, -sine), (minus, -sine, sine)):
                r, c = row * width, col * width
                ref[r : r + tile, c : c + tile] = cosine
                ref[r + tile : r + width, c + tile : c + width] = cosine
                ref[r : r + tile, c + tile : c + width] = upper
                ref[r + tile : r + width, c : c + tile] = lower


def front_kernel(
    peers, shape, base_ref, probe_ref, patch_ref, amp_ref, dir_ref, pre_ref, sums_ref,
    plus, minus, probe, exits, wave, stacked, own, other, load_sem, send_sem, recv_sem,
    lit, held_i, tile_in, tile_all, grad, light_own, prev, sums_in, sums_all, *rest,
):
    islots, isc_s, isc_r, (icore_s, icore_r, ibc_s, ibc_r) = rest[0:4], rest[4:8], rest[8:12], rest[12:16]
    (core_s, core_r), sc_s, sc_r, ga_s, ga_r = rest[16:18], rest[18:22], rest[22:26], rest[26:30], rest[30:34]
    back_s, back_r, dir_sem, bc_s, bc_r, out_sem, ready = rest[34:]
    spot = Spot(*shape)
    positions, modes = exits.shape[0], exits.shape[1]
    width = base_ref.shape[1]
    tile = width // 2
    step = min(64, tile)
    f32, bf16 = jnp.float32, jnp.bfloat16
    y = lax.axis_index("mode")
    share = Shares(spot, width)
    pixels = float(width * width)

    barrier = pltpu.get_barrier_semaphore()
    for k in range(1, peers):
        pl.semaphore_signal(barrier, inc=1, device_id={"mode": lax.rem(y + k, peers)}, device_id_type=MESH)
    for k in range(1, spot.count):
        to = lax.rem(spot.me + k, spot.count)
        pl.semaphore_signal(barrier, inc=1, device_id={"grp": to}, device_id_type=MESH)

    def load(m):
        return pltpu.make_async_copy(probe_ref.at[:, m], probe.at[m], load_sem.at[m])

    for m in range(modes):
        load(m).start()
    def load_prev(path, m):
        start = pl.multiple_of(share.base + share.offset[path], 8)
        return pltpu.make_async_copy(dir_ref.at[:, m, pl.ds(start, share.own), :], prev.at[m], dir_sem.at[m])

    def fetch(path):
        for m in range(modes):
            load_prev(path, m).start()

    per_path(spot, shape[2], fetch)
    sums_in[...] = jnp.zeros_like(sums_in)
    build_tables(base_ref, plus, minus)
    pl.semaphore_wait(barrier, peers - 1 + spot.count - 1)

    def swap(p, t, k):
        rows = pl.ds(t * tile, tile)
        return remote(
            own.at[p, rows], other.at[k - 1, p, rows], send_sem.at[k - 1, p, t], recv_sem.at[k - 1, p, t],
            {"mode": lax.rem(y + k, peers)},
        )

    def put(half, m, rows):
        for col in range(2):
            for part in range(2):
                block = half[:, (2 * col + part) * tile : (2 * col + part + 1) * tile]
                stacked[m, pl.ds(rows * width + part * tile, tile), col * tile : (col + 1) * tile] = block

    def leave(p, m):
        def body(i, carry):
            rows = pl.ds(pl.multiple_of(i * step, step), step)
            for col in range(2):
                at = pl.ds(col * tile, tile)
                obj_re = patch_ref[p, 0, rows, at].astype(f32)
                obj_im = patch_ref[p, 1, rows, at].astype(f32)
                pro_re, pro_im = probe[m, 0, rows, at], probe[m, 1, rows, at]
                exits[p, m, rows, 2 * col * tile : (2 * col + 1) * tile] = (pro_re * obj_re - pro_im * obj_im).astype(bf16)
                exits[p, m, rows, (2 * col + 1) * tile : (2 * col + 2) * tile] = (pro_re * obj_im + pro_im * obj_re).astype(bf16)
            return carry

        lax.fori_loop(0, width // step, body, 0)

    def forward(p, carry):
        def first(m, carry):
            @pl.when(p == 0)
            def _():
                load(m).wait()

            leave(p, m)
            half = jnp.dot(exits[p, m], plus[...], preferred_element_type=f32).astype(bf16)
            for rows in range(2):
                put(half[rows * tile : (rows + 1) * tile], m, rows)
            return carry

        lax.fori_loop(0, modes, first, 0)
        for t in range(2):
            rows = pl.ds(t * tile, tile)

            def second(m, carry):
                out = jnp.dot(minus[t * width : (t + 1) * width, :], stacked[m], preferred_element_type=f32)
                real, imag = out[:tile], out[tile:]
                wave[p, m, t, 0] = real
                wave[p, m, t, 1] = imag
                light = real * real + imag * imag
                own[p, rows, :] = jnp.where(m == 0, light, own[p, rows, :] + light)
                return carry

            lax.fori_loop(0, modes, second, 0)
            for k in range(1, peers):
                swap(p, t, k).start()
        return carry

    lax.fori_loop(0, positions, forward, 0)

    def give_light():
        away = rows_at(lit, (1 - spot.core) * share.part, share.part)
        return remote(away, held_i, icore_s.at[0], icore_r.at[0], spot.partner())

    def shine(i, carry):
        rows = pl.ds(pl.multiple_of(i * step, step), step)
        acc = jnp.zeros((step, width), f32)
        for p in range(positions):
            obj_re, obj_im = patch_ref[p, 0, rows, :].astype(f32), patch_ref[p, 1, rows, :].astype(f32)
            acc = acc + obj_re * obj_re + obj_im * obj_im
        lit[0, rows, :] = acc
        return carry

    def spare(k, slot):
        return islots[k].at[slot]

    def light_parts(path):
        sems = [(functools.partial(spare, k), isc_s[k], isc_r[k]) for k in (2 * path, 2 * path + 1)]
        return share.scatter_parts(path, held_i, sems)

    def light_scatter(path):
        for line, chunk, slot, send, recv in light_parts(path):
            for _ in line.scatter(chunk, slot, send, recv):
                pass
        block = held_i[0, pl.ds(pl.multiple_of(share.offset[path], 8), share.own), :]
        light_own[...] = block
        tile_in[...] = fold_lanes(block)

    def light_end(path):
        for line, chunk, slot, send, recv in light_parts(path):
            line.scatter_end(chunk, slot, send, recv)

    lax.fori_loop(0, width // step, shine, 0)
    give_light().start()
    give_light().wait_recv()
    add_rows(held_i, lit, share.base, share.part)
    per_path(spot, shape[2], light_scatter)
    for copy in broadcast(spot, tile_in, tile_all, ibc_s, ibc_r):
        copy.start()
    tile_all[0] = tile_in[...]

    def unfix(p):
        for t in range(2):
            for k in range(1, peers):
                swap(p, t, k).wait_recv()

            def scale(i, carry):
                rows = pl.ds(pl.multiple_of(t * tile + i * step, step), step)
                total = own[p, rows, :]
                for k in range(peers - 1):
                    total = total + other[k, p, rows, :]
                ratio = amp_ref[p, rows, :].astype(f32) / jnp.sqrt(total + 1.0)
                here = pl.ds(pl.multiple_of(i * step, step), step)

                def fix(m, carry):
                    for part in range(2):
                        wave[p, m, t, part, here, :] = wave[p, m, t, part, here, :] * ratio
                    return carry

                lax.fori_loop(0, modes, fix, 0)
                return carry

            lax.fori_loop(0, tile // step, scale, 0)

            def first(m, carry):
                fixed = [wave[p, m, t, part].astype(bf16) for part in range(2)]
                blocks = [fixed[part][:, col * tile : (col + 1) * tile] for col in range(2) for part in range(2)]
                joined = jnp.concatenate(blocks, axis=1)
                half = jnp.dot(joined, minus[...], preferred_element_type=f32).astype(bf16)
                put(half, m, t)
                return carry

            lax.fori_loop(0, modes, first, 0)

    def gradient(p, m):
        for t in range(2):
            rows = pl.ds(t * tile, tile)
            out = jnp.dot(plus[t * width : (t + 1) * width, :], stacked[m], preferred_element_type=f32)
            for col in range(2):
                at = pl.ds(col * tile, tile)
                real, imag = out[:tile, col * tile : (col + 1) * tile], out[tile:, col * tile : (col + 1) * tile]
                obj_re = patch_ref[p, 0, rows, at].astype(f32)
                obj_im = patch_ref[p, 1, rows, at].astype(f32)
                diff_re = real - exits[p, m, rows, 2 * col * tile : (2 * col + 1) * tile].astype(f32)
                diff_im = imag - exits[p, m, rows, (2 * col + 1) * tile : (2 * col + 2) * tile].astype(f32)
                add_re = obj_re * diff_re + obj_im * diff_im
                add_im = obj_re * diff_im - obj_im * diff_re
                grad[m, 0, rows, at] = jnp.where(p == 0, add_re, grad[m, 0, rows, at] + add_re)
                grad[m, 1, rows, at] = jnp.where(p == 0, add_im, grad[m, 1, rows, at] + add_im)

    def backward(p, carry):
        unfix(p)

        def one(m, carry):
            gradient(p, m)
            return carry

        lax.fori_loop(0, modes, one, 0)
        return carry

    last = positions - 1
    lax.fori_loop(0, last, backward, 0)
    unfix(last)
    for k in range(1, spot.count):
        pl.semaphore_signal(ready, inc=1, device_id={"grp": lax.rem(spot.me + k, spot.count)}, device_id_type=MESH)
    for copy in broadcast(spot, tile_in, tile_all, ibc_s, ibc_r):
        copy.wait()
    shift = jnp.sum(tile_all[...]) / pixels

    def held(m):
        return wave.at[0, m, 0]

    def room(m, k, slot):
        rows = scatter_sizes(shape, width)[k][1]
        at = slot * rows + tile
        if k % 2:
            return wave.at[1, m, 1, :, pl.ds(pl.multiple_of(slot * rows, 8), rows), :]
        block = at // tile
        rem = (lambda a, b: a % b) if isinstance(slot, int) else lax.rem
        return wave.at[block // 2, m, rem(block, 2), :, pl.ds(pl.multiple_of(rem(at, tile), 8), rows), :]

    def give(m):
        other = (1 - spot.core) * share.part
        return remote(
            rows_at(grad.at[m], other, share.part), held(m), core_s.at[m], core_r.at[m], spot.partner()
        )

    def scatter_parts(m, path):
        sems = [(functools.partial(room, m, k), sc_s[k].at[m], sc_r[k].at[m]) for k in (2 * path, 2 * path + 1)]
        return share.scatter_parts(path, held(m), sems)

    def gather_parts(m, path):
        sems = [(ga_s[k].at[m], ga_r[k].at[m]) for k in (2 * path, 2 * path + 1)]
        return share.gather_parts(path, probe.at[m], sems)

    def home(m):
        block = rows_at(probe.at[m], share.base, share.part)
        return remote(block, block, back_s.at[m], back_r.at[m], spot.partner())

    def stream(m, path):
        give(m).wait_recv()
        add_rows(held(m), grad.at[m], share.base, share.part)
        for line, chunk, slot, send, recv in scatter_parts(m, path):
            yield from line.scatter(chunk, slot, send, recv)
        rows = pl.ds(pl.multiple_of(share.offset[path], 8), share.own)
        to = pl.ds(pl.multiple_of(share.base + share.offset[path], 8), share.own)
        light = light_own[...]
        load_prev(path, m).wait()
        g_re, g_im = held(m)[0, rows, :], held(m)[1, rows, :]
        d_re, d_im = prev[m, 0], prev[m, 1]
        den = light + shift
        p_re, p_im = g_re / den, g_im / den
        probe[m, 0, to, :] = p_re
        probe[m, 1, to, :] = p_im
        (line, chunk, send, recv), later = gather_parts(m, path)
        walk = line.gather(chunk, send, recv)
        next(walk, None)
        terms = (
            g_re * p_re + g_im * p_im,
            g_re * d_re + g_im * d_im,
            light * (p_re * p_re + p_im * p_im),
            light * (p_re * d_re + p_im * d_im),
            light * (d_re * d_re + d_im * d_im),
        )
        for k, term in enumerate(terms):
            row = 5 * m + k
            sums_in[row : row + 1, :] = jnp.sum(fold_lanes(term), axis=0, keepdims=True)
        yield
        yield from walk
        line, chunk, send, recv = later
        yield from line.gather(chunk, send, recv)
        home(m).start()

    streams = [[stream(m, path) for m in range(modes)] for path in range(2)]
    orders = [list(turns(shape, modes, path)) for path in range(2)]

    def advance(path):
        order = orders[path]
        while order and order[0] != modes:
            next(streams[path][order.pop(0)], None)

    for m in range(modes):
        gradient(last, m)
        if m == 0:
            pl.semaphore_wait(ready, spot.count - 1)
        give(m).start()
        for path in range(2):
            orders[path].pop(0)
        per_path(spot, shape[2], advance)
    for copy in broadcast(spot, sums_in, sums_all, bc_s, bc_r):
        copy.start()
    sums_all[0] = sums_in[...]

    def out(m):
        return pltpu.make_async_copy(probe.at[m], pre_ref.at[m], out_sem.at[m])

    for m in range(modes):
        home(m).wait_recv()
        out(m).start()
    for copy in broadcast(spot, sums_in, sums_all, bc_s, bc_r):
        copy.wait()
    sums_ref[...] = jnp.sum(sums_all[...], axis=0)

    def close(path):
        light_end(path)
        for m in range(modes):
            for line, chunk, slot, send, recv in scatter_parts(m, path):
                line.scatter_end(chunk, slot, send, recv)
            for line, chunk, send, recv in gather_parts(m, path):
                line.gather_end(chunk, send, recv)

    give_light().wait_send()
    for m in range(modes):
        give(m).wait_send()
        home(m).wait_send()
    per_path(spot, shape[2], close)
    for m in range(modes):
        out(m).wait()
    for p in range(positions):
        for t in range(2):
            for k in range(1, peers):
                swap(p, t, k).wait_send()


def front(base, probe, patches, amplitude, direction):
    modes, width = probe.shape[1], probe.shape[2]
    positions = patches.shape[0]
    peers = lax.axis_size("mode")
    tile = width // 2
    dma = pltpu.SemaphoreType.DMA
    f32, bf16 = jnp.float32, jnp.bfloat16
    vmem = pl.BlockSpec(memory_space=pltpu.VMEM)
    shape = split_lines(lax.axis_size("grp"))
    outer, inner, cores = shape
    assert cores == 2 and positions >= 2
    sizes = scatter_sizes(shape, width)
    count, lanes = lax.axis_size("grp"), min(128, width)
    own = sizes[1][1]
    back_sizes = [outer, inner, inner, outer]
    sum_rows = -(-5 * modes // 8) * 8
    hbm = pl.BlockSpec(memory_space=pl.ANY)
    flops = positions * modes * 2 * 16 * width**3
    return pl.pallas_call(
        functools.partial(front_kernel, peers, shape),
        in_specs=[vmem, hbm, vmem, vmem, hbm],
        out_specs=[hbm, vmem],
        out_shape=[
            jax.ShapeDtypeStruct((modes, 2, width, width), f32),
            jax.ShapeDtypeStruct((sum_rows, lanes), f32),
        ],
        scratch_shapes=[
            pltpu.VMEM((2 * width, 2 * width), bf16),
            pltpu.VMEM((2 * width, 2 * width), bf16),
            pltpu.VMEM((modes, 2, width, width), f32),
            pltpu.VMEM((positions, modes, width, 2 * width), bf16),
            pltpu.VMEM((positions, modes, 2, 2, tile, width), f32),
            pltpu.VMEM((modes, 2 * width, width), bf16),
            pltpu.VMEM((positions, width, width), f32),
            pltpu.VMEM((max(peers - 1, 1), positions, width, width), f32),
            dma((modes,)),
            dma((max(peers - 1, 1), positions, 2)),
            dma((max(peers - 1, 1), positions, 2)),
            pltpu.VMEM((1, width, width), f32),
            pltpu.VMEM((1, width // shape[2], width), f32),
            pltpu.VMEM((8, lanes), f32),
            pltpu.VMEM((count, 8, lanes), f32),
            pltpu.VMEM((modes, 2, width, width), f32),
            pltpu.VMEM((own, width), f32),
            pltpu.VMEM((modes, 2, own, width), f32),
            pltpu.VMEM((sum_rows, lanes), f32),
            pltpu.VMEM((count, sum_rows, lanes), f32),
            *[pltpu.VMEM((n + 1, 1, rows, width), f32) for n, rows in sizes],
            *[dma((n,)) for n, _ in sizes],
            *[dma((n + 1,)) for n, _ in sizes],
            dma((1,)),
            dma((1,)),
            dma((count,)),
            dma((count,)),
            dma((modes,)),
            dma((modes,)),
            *[dma((modes, n)) for n, _ in sizes],
            *[dma((modes, n + 1)) for n, _ in sizes],
            *[dma((modes, 2, n)) for n in back_sizes],
            *[dma((modes, n)) for n in back_sizes],
            dma((modes,)),
            dma((modes,)),
            dma((modes,)),
            dma((count,)),
            dma((count,)),
            dma((modes,)),
            pltpu.SemaphoreType.REGULAR,
        ],
        compiler_params=pltpu.CompilerParams(collective_id=1, has_side_effects=True, vmem_limit_bytes=FRONT_LIMIT),
        cost_estimate=pl.CostEstimate(flops=flops, bytes_accessed=0, transcendentals=0),
        name="front",
    )(base, probe, patches, amplitude, direction)


def split_lines(count):
    cores = 2 if count % 2 == 0 else 1
    chips = count // cores
    inner = 1
    while inner * inner * 4 <= chips and chips % (inner * 2) == 0:
        inner *= 2
    return chips // inner, inner, cores


class Shares:
    def __init__(self, spot, width):
        outer, inner, cores = spot.sizes
        self.part = width // cores
        self.own = self.part // (outer * inner)
        self.base = spot.core * self.part
        self.big = (self.part // inner, self.part // outer)
        first = Line(spot, "inner", inner, spot.inner)
        second = Line(spot, "outer", outer, spot.outer)
        self.lines = ((first, second), (second, first))
        self.group = (spot.inner * self.big[0], spot.outer * self.big[1])
        self.offset = (self.group[0] + spot.outer * self.own, self.group[1] + spot.inner * self.own)

    def scatter_parts(self, path, held, sems):
        top = lambda k: rows_at(held, k * self.big[path], self.big[path])
        low = lambda k: rows_at(held, self.group[path] + k * self.own, self.own)
        return [(line, chunk) + pair for line, chunk, pair in zip(self.lines[path], (top, low), sems)]

    def gather_parts(self, path, whole_ref, sems):
        low = lambda k: rows_at(whole_ref, self.base + self.group[path] + k * self.own, self.own)
        top = lambda k: rows_at(whole_ref, self.base + k * self.big[path], self.big[path])
        return [(line, chunk) + pair for line, chunk, pair in zip(self.lines[path][::-1], (low, top), sems)]


def rows_at(ref, start, count):
    return ref.at[:, pl.ds(pl.multiple_of(start, 8), count), :]


def scatter_sizes(shape, width):
    outer, inner, cores = shape
    part = width // cores
    own = part // (outer * inner)
    return [(inner, part // inner), (outer, own), (outer, part // outer), (inner, own)]


def add_rows(into, mine, start, count):
    step = 32 if count % 32 == 0 else count

    def add(i, carry):
        rows = pl.ds(pl.multiple_of(i * step, 8), step)
        into[:, rows, :] += mine[:, pl.ds(pl.multiple_of(start + i * step, 8), step), :]
        return carry

    lax.fori_loop(0, count // step, add, 0)


def broadcast(spot, src, dst, send, recv):
    copies = []
    for step in range(1, spot.count):
        to = lax.rem(spot.me + step, spot.count)
        copies.append(remote(src, dst.at[step], send.at[step], recv.at[step], {"grp": to}))
    return copies


def per_path(spot, count, act):
    for path in range(count):
        @pl.when(spot.core == path)
        def _():
            act(path)


def turns(shape, modes, path):
    key = (*shape, modes)
    if key in ORDERS:
        return ORDERS[key][path]
    steps = 8 * (shape[0] + shape[1])
    events = sorted((k + (3 * m) // 2, m) for m in range(modes) for k in range(steps))
    return [modes] * modes + [m for _, m in events]


def finish_kernel(norm_ref, sums_ref, pre_ref, probe_ref, dir_ref, new_probe, new_dir, new_norm, kept):
    mode = pl.program_id(0)
    pixels = float(new_probe.shape[3] ** 2)

    @pl.when(pl.program_id(1) == 0)
    def _():
        index = lax.broadcasted_iota(jnp.int32, sums_ref.shape, 0)

        def mean(k):
            return jnp.sum(jnp.where(index == 5 * mode + k, sums_ref[...], 0.0)) / pixels

        norm, cross, light, light_cross, light_prev = (mean(k) for k in range(5))
        new_norm[mode] = norm
        beta = norm / norm_ref[mode]
        upper = norm + beta * cross
        lower = light + beta * (2.0 * light_cross + beta * light_prev)
        kept[0] = beta
        kept[1] = upper / (lower + 1.0)

    beta, alpha = kept[0], kept[1]
    rows = new_probe.shape[2]
    small = min(32, rows)

    def body(i, carry):
        at = pl.ds(pl.multiple_of(i * small, small), small)
        for part in range(2):
            step = pre_ref[0, part, at, :] + beta * dir_ref[part, 0, at, :]
            new_dir[part, 0, at, :] = step
            new_probe[part, 0, at, :] = probe_ref[part, 0, at, :] + alpha * step
        return carry

    lax.fori_loop(0, rows // small, body, 0)


def finish(prev_norm, sums, pre, probe, direction):
    modes, width = probe.shape[1], probe.shape[2]
    rows = min(256, width)
    block = pl.BlockSpec((2, 1, rows, width), lambda m, r: (0, m, r, 0))
    smem = pl.BlockSpec(memory_space=pltpu.SMEM)
    return pl.pallas_call(
        finish_kernel,
        grid=(modes, width // rows),
        in_specs=[
            smem,
            whole(sums.shape),
            pl.BlockSpec((1, 2, rows, width), lambda m, r: (m, 0, r, 0)),
            block,
            block,
        ],
        out_specs=[block, block, smem],
        out_shape=[
            jax.ShapeDtypeStruct(probe.shape, jnp.float32),
            jax.ShapeDtypeStruct(probe.shape, jnp.float32),
            jax.ShapeDtypeStruct((modes,), jnp.float32),
        ],
        scratch_shapes=[pltpu.SMEM((2,), jnp.float32)],
        compiler_params=pltpu.CompilerParams(
            dimension_semantics=("arbitrary", "arbitrary"), vmem_limit_bytes=FINISH_LIMIT
        ),
        name="finish",
    )(prev_norm, sums, pre, probe, direction)


def cut_kernel(offset_ref, tile_ref, patch_ref, wide):
    positions, width, full = patch_ref.shape[0], patch_ref.shape[2], tile_ref.shape[2]
    step = 64 if width % 64 == 0 else width

    def widen(i, carry):
        rows = pl.ds(pl.multiple_of(i * step, step), step)
        for part in range(2):
            wide[part, rows, :] = tile_ref[part, rows, :].astype(jnp.float32)
        return carry

    lax.fori_loop(0, full // step, widen, 0)

    def position(p, carry):
        row, col = offset_ref[p, 0], offset_ref[p, 1]
        turn = lax.rem(full - col, full)
        low = lax.rem(row, 8)
        lift = lax.rem(step + 8 - low, step + 8)

        def body(i, carry):
            for part in range(2):
                block = wide[part, pl.ds(pl.multiple_of(row - low + i * step, 8), step + 8), :]
                block = pltpu.roll(pltpu.roll(block, lift, 0)[:step], turn, 1)[:, :width]
                patch_ref[p, part, pl.ds(pl.multiple_of(i * step, step), step), :] = block.astype(jnp.bfloat16)
            return carry

        lax.fori_loop(0, width // step, body, 0)
        return carry

    lax.fori_loop(0, positions, position, 0)


def cut(offsets, tile, width):
    positions = offsets.shape[0]
    vmem = pl.BlockSpec(memory_space=pltpu.VMEM)
    return pl.pallas_call(
        cut_kernel,
        in_specs=[pl.BlockSpec(memory_space=pltpu.SMEM), vmem],
        out_specs=vmem,
        out_shape=jax.ShapeDtypeStruct((positions, 2, width, width), jnp.bfloat16),
        scratch_shapes=[pltpu.VMEM((2, tile.shape[1] + 8, tile.shape[2]), jnp.float32)],
        compiler_params=pltpu.CompilerParams(vmem_limit_bytes=CUT_LIMIT),
        name="cut",
    )(offsets, tile)


def whole(shape):
    return pl.BlockSpec(shape, lambda *_: (0,) * len(shape))


def on_device(probe, prev_direction, prev_norm, object_tile, offsets, amplitude):
    width = probe.shape[2]
    patches = cut(offsets, object_tile, width)
    pre, sums = front(base_table(width), probe, patches, amplitude, prev_direction)
    return tuple(finish(prev_norm, sums, pre, probe, prev_direction))


def solution(mesh):
    return jax.shard_map(
        on_device,
        mesh=mesh,
        in_specs=(
            P(None, "mode", None, None),
            P(None, "mode", None, None),
            P("mode"),
            P(None, "grp", None),
            P("grp", None),
            P("grp", None, None),
        ),
        out_specs=(P(None, "mode", None, None), P(None, "mode", None, None), P("mode")),
        check_vma=False,
    )
```

```python
import functools
import math

import jax
import numpy as np
import jax.numpy as jnp
from jax import lax
from jax.experimental import pallas as pl
from jax.experimental.pallas import tpu as pltpu
from jax.sharding import PartitionSpec as P

MESH = pl.DeviceIdType.MESH
VMEM_LIMIT = 60 * 1024 * 1024
FRONT_LIMIT = 67043328
CUT_LIMIT = 16 * 1024 * 1024
FINISH_LIMIT = 60 * 1024 * 1024
ORDERS = {
    (4, 2, 2, 4): (
        (
            4, 4, 0, 4, 1, 4, 2, 0, 1, 1, 0, 3, 0, 1, 1, 1, 0, 0, 1, 2, 1, 0, 3, 0, 3, 2, 1, 3, 3,
            3, 0, 2, 1, 1, 2, 2, 0, 0, 1, 2, 3, 3, 2, 0, 3, 0, 2, 2, 3, 1, 1, 0, 2, 3, 2, 2, 3, 3,
            1, 3, 0, 2, 3, 2,
        ),
        (
            4, 4, 0, 4, 1, 0, 0, 4, 1, 0, 2, 3, 0, 0, 2, 0, 1, 3, 0, 2, 1, 0, 1, 1, 0, 2, 2, 0, 2,
            1, 0, 1, 2, 3, 3, 1, 3, 2, 0, 2, 3, 1, 3, 3, 2, 1, 2, 1, 3, 0, 3, 2, 1, 0, 2, 3, 2, 1,
            3, 1, 2, 3, 3, 3,
        ),
    ),
}


def base_table(width):
    index = np.arange(width, dtype=np.int64)
    product = index[:, None] * index[None, :] % width
    angle = np.float32(-2.0 * math.pi / width) * product.astype(np.float32)
    scale = np.float32(1.0 / math.sqrt(width))
    both = np.stack([np.cos(angle) * scale, np.sin(angle) * scale])
    return jnp.asarray(both.astype(jnp.bfloat16))


def fold_lanes(block):
    rows, width = block.shape
    lanes = min(128, width)
    acc = jnp.sum(block.reshape(rows // 8, 8, width), axis=0)
    out = acc[:, :lanes]
    for at in range(lanes, width, lanes):
        out = out + acc[:, at : at + lanes]
    return out


class Spot:
    def __init__(self, outer, inner, cores):
        me = lax.axis_index("grp")
        self.me = me
        self.sizes = (outer, inner, cores)
        self.count = outer * inner * cores
        self.core = lax.rem(me, cores)
        self.inner = lax.rem(me // cores, inner)
        self.outer = me // (cores * inner)
        self.stride = {"core": 1, "inner": cores, "outer": cores * inner}

    def at(self, line, step):
        return {"grp": self.me + step * self.stride[line]}

    def partner(self):
        return {"grp": self.me + 1 - 2 * self.core}


def remote(src, dst, send, recv, device):
    return pltpu.make_async_remote_copy(
        src_ref=src, dst_ref=dst, send_sem=send, recv_sem=recv, device_id=device, device_id_type=MESH
    )


class Line:
    def __init__(self, spot, name, length, place):
        self.spot, self.name, self.length, self.place = spot, name, length, place

    def scatter(self, chunk, slots, send, recv):
        size, u = self.length, self.place

        def take(slot, into):
            got = remote(slots(slot), slots(slot), send().at[0], recv().at[slot], self.spot.at(self.name, 0))
            got.wait_recv()
            into[...] += slots(slot)[...]

        def push(k, step, slot):
            remote(chunk(k), slots(slot), send().at[k], recv().at[slot], self.spot.at(self.name, step)).start()

        for step in range(size - 1):
            right, left = size - 1 - step, step

            @pl.when(u < right)
            def _():
                @pl.when(u > 0)
                def _():
                    take(right + 1, chunk(right))

                push(right, 1, right + 1)

            if size > 2:
                yield

            @pl.when(u > left)
            def _():
                @pl.when(u < size - 1)
                def _():
                    take(left, chunk(left))

                push(left, -1, left)

            yield

        @pl.when(u > 0)
        def _():
            take(u + 1, chunk(u))

        @pl.when(u < size - 1)
        def _():
            take(u, chunk(u))

    def scatter_end(self, chunk, slots, send, recv):
        for k in range(self.length):
            @pl.when(self.place != k)
            def _():
                remote(chunk(k), slots(0), send().at[k], recv().at[0], self.spot.at(self.name, 0)).wait_send()

    def gather(self, chunk, send, recv):
        size, u = self.length, self.place

        def push(k, way, step):
            remote(chunk(k), chunk(k), send().at[way, k], recv().at[k], self.spot.at(self.name, step)).start()

        def take(k):
            remote(chunk(k), chunk(k), send().at[0, 0], recv().at[k], self.spot.at(self.name, 0)).wait_recv()

        for step in range(size):
            low = u - step

            @pl.when(low >= 0)
            def _():
                if step > 0:
                    take(low)

                @pl.when(u < size - 1)
                def _():
                    push(low, 0, 1)

            if size > 2 and step > 0:
                yield
            high = u + step

            @pl.when(high < size)
            def _():
                if step > 0:
                    take(high)

                @pl.when(u > 0)
                def _():
                    push(high, 1, -1)

            if step < size - 1:
                yield

    def gather_end(self, chunk, send, recv):
        size, u = self.length, self.place
        for k in range(size):
            for way in range(2):
                @pl.when((u < size - 1) & (u >= k) if way == 0 else (u > 0) & (u <= k))
                def _():
                    remote(chunk(k), chunk(k), send().at[way, k], recv().at[k], self.spot.at(self.name, 0)).wait_send()


def build_tables(base_ref, plus, minus):
    width = base_ref.shape[1]
    tile = width // 2
    for row in range(2):
        for col in range(2):
            take = (pl.ds(row * tile, tile), pl.ds(col * tile, tile))
            cosine, sine = base_ref[(0, *take)], base_ref[(1, *take)]
            for ref, upper, lower in ((plus, sine, -sine), (minus, -sine, sine)):
                r, c = row * width, col * width
                ref[r : r + tile, c : c + tile] = cosine
                ref[r + tile : r + width, c + tile : c + width] = cosine
                ref[r : r + tile, c + tile : c + width] = upper
                ref[r + tile : r + width, c : c + tile] = lower


def pick(ref, *index):
    return (lambda: ref.at[index]) if index else (lambda: ref)


def front_kernel(
    peers, shape, base_ref, probe_ref, patch_ref, amp_hbm, dir_ref, pre_ref, sums_ref,
    plus, minus, probe, exits, wave, stacked, own, other, load_sem, send_sem, recv_sem,
    lit, held_i, tile_in, tile_all, grad, light_own, prev, sums_in, sums_all, *rest,
):
    islots, isc_s, isc_r, (icore_s, icore_r, ibc_s, ibc_r) = rest[0:4], rest[4:8], rest[8:12], rest[12:16]
    (core_s, core_r), sc_s, sc_r, ga_s, ga_r = rest[16:18], rest[18:22], rest[22:26], rest[26:30], rest[30:34]
    back_s, back_r, dir_sem, bc_s, bc_r, out_sem, ready, amp_ref, amp_sem = rest[34:]
    spot = Spot(*shape)
    positions, modes = exits.shape[0], exits.shape[1]
    width = base_ref.shape[1]
    tile = width // 2
    step = min(64, tile)
    f32, bf16 = jnp.float32, jnp.bfloat16
    y = lax.axis_index("mode")
    share = Shares(spot, width)
    pixels = float(width * width)

    barrier = pltpu.get_barrier_semaphore()
    for k in range(1, peers):
        pl.semaphore_signal(barrier, inc=1, device_id={"mode": lax.rem(y + k, peers)}, device_id_type=MESH)
    for k in range(1, spot.count):
        to = lax.rem(spot.me + k, spot.count)
        pl.semaphore_signal(barrier, inc=1, device_id={"grp": to}, device_id_type=MESH)

    def load(m):
        return pltpu.make_async_copy(probe_ref.at[:, m], probe.at[m], load_sem.at[m])

    for m in range(modes):
        load(m).start()
    amp_load = pltpu.make_async_copy(amp_hbm, amp_ref, amp_sem.at[0])
    amp_load.start()
    def load_prev(path, m):
        start = pl.multiple_of(share.base + share.offset[path], 8)
        return pltpu.make_async_copy(dir_ref.at[:, m, pl.ds(start, share.own), :], prev.at[m], dir_sem.at[m])

    def fetch(path):
        for m in range(modes):
            load_prev(path, m).start()

    per_path(spot, shape[2], fetch)
    sums_in[...] = jnp.zeros_like(sums_in)
    build_tables(base_ref, plus, minus)

    def swap(p, t, k):
        rows = pl.ds(t * tile, tile)
        return remote(
            own.at[p, rows], other.at[k - 1, p, rows], send_sem.at[k - 1, p, t], recv_sem.at[k - 1, p, t],
            {"mode": lax.rem(y + k, peers)},
        )

    def put(half, m, rows):
        for col in range(2):
            for part in range(2):
                block = half[:, (2 * col + part) * tile : (2 * col + part + 1) * tile]
                stacked[m, pl.ds(rows * width + part * tile, tile), col * tile : (col + 1) * tile] = block

    def leave(p, m):
        def body(i, carry):
            rows = pl.ds(pl.multiple_of(i * step, step), step)
            for col in range(2):
                at = pl.ds(col * tile, tile)
                obj_re = patch_ref[p, 0, rows, at].astype(f32)
                obj_im = patch_ref[p, 1, rows, at].astype(f32)
                pro_re, pro_im = probe[m, 0, rows, at], probe[m, 1, rows, at]
                exits[p, m, rows, 2 * col * tile : (2 * col + 1) * tile] = (pro_re * obj_re - pro_im * obj_im).astype(bf16)
                exits[p, m, rows, (2 * col + 1) * tile : (2 * col + 2) * tile] = (pro_re * obj_im + pro_im * obj_re).astype(bf16)
            return carry

        lax.fori_loop(0, width // step, body, 0)

    def forward(p, carry):
        def first(m, carry):
            @pl.when(p == 0)
            def _():
                load(m).wait()

            leave(p, m)
            half = jnp.dot(exits[p, m], plus[...], preferred_element_type=f32).astype(bf16)
            for rows in range(2):
                put(half[rows * tile : (rows + 1) * tile], m, rows)
            return carry

        lax.fori_loop(0, modes, first, 0)
        for t in range(2):
            rows = pl.ds(t * tile, tile)

            def second(m, carry):
                out = jnp.dot(minus[t * width : (t + 1) * width, :], stacked[m], preferred_element_type=f32)
                real, imag = out[:tile], out[tile:]
                wave[p, m, t, 0] = real
                wave[p, m, t, 1] = imag
                light = real * real + imag * imag
                own[p, rows, :] = jnp.where(m == 0, light, own[p, rows, :] + light)
                return carry

            lax.fori_loop(0, modes, second, 0)
            if t == 0:
                @pl.when(p == 0)
                def _():
                    pl.semaphore_wait(barrier, peers - 1 + spot.count - 1)

            for k in range(1, peers):
                swap(p, t, k).start()
        return carry

    lax.fori_loop(0, positions, forward, 0)

    def give_light():
        away = rows_at(lit, (1 - spot.core) * share.part, share.part)
        return remote(away, held_i, icore_s.at[0], icore_r.at[0], spot.partner())

    def shine(i, carry):
        rows = pl.ds(pl.multiple_of(i * step, step), step)
        acc = jnp.zeros((step, width), f32)
        for p in range(positions):
            obj_re, obj_im = patch_ref[p, 0, rows, :].astype(f32), patch_ref[p, 1, rows, :].astype(f32)
            acc = acc + obj_re * obj_re + obj_im * obj_im
        lit[0, rows, :] = acc
        return carry

    def spare(k, slot):
        return islots[k].at[slot]

    def light_parts(path):
        sems = [(functools.partial(spare, k), pick(isc_s[k]), pick(isc_r[k])) for k in (2 * path, 2 * path + 1)]
        return share.scatter_parts(path, pick(held_i), sems)

    def light_scatter(path):
        for line, chunk, slot, send, recv in light_parts(path):
            for _ in line.scatter(chunk, slot, send, recv):
                pass
        block = held_i[0, pl.ds(pl.multiple_of(share.offset[path], 8), share.own), :]
        light_own[...] = block
        tile_in[...] = fold_lanes(block)

    def light_end(path):
        for line, chunk, slot, send, recv in light_parts(path):
            line.scatter_end(chunk, slot, send, recv)

    lax.fori_loop(0, width // step, shine, 0)
    give_light().start()
    give_light().wait_recv()
    add_rows(held_i, lit, share.base, share.part)
    per_path(spot, shape[2], light_scatter)
    for copy in broadcast(spot, tile_in, tile_all, ibc_s, ibc_r):
        copy.start()
    tile_all[0] = tile_in[...]

    def unfix(p):
        for t in range(2):
            for k in range(1, peers):
                swap(p, t, k).wait_recv()

            def scale(i, carry):
                rows = pl.ds(pl.multiple_of(t * tile + i * step, step), step)
                total = own[p, rows, :]
                for k in range(peers - 1):
                    total = total + other[k, p, rows, :]
                ratio = amp_ref[p, rows, :].astype(f32) / jnp.sqrt(total + 1.0)
                here = pl.ds(pl.multiple_of(i * step, step), step)

                def fix(m, carry):
                    for part in range(2):
                        wave[p, m, t, part, here, :] = wave[p, m, t, part, here, :] * ratio
                    return carry

                lax.fori_loop(0, modes, fix, 0)
                return carry

            lax.fori_loop(0, tile // step, scale, 0)

            def first(m, carry):
                fixed = [wave[p, m, t, part].astype(bf16) for part in range(2)]
                blocks = [fixed[part][:, col * tile : (col + 1) * tile] for col in range(2) for part in range(2)]
                joined = jnp.concatenate(blocks, axis=1)
                half = jnp.dot(joined, minus[...], preferred_element_type=f32).astype(bf16)
                put(half, m, t)
                return carry

            lax.fori_loop(0, modes, first, 0)

    def gradient(p, m):
        for t in range(2):
            rows = pl.ds(t * tile, tile)
            out = jnp.dot(plus[t * width : (t + 1) * width, :], stacked[m], preferred_element_type=f32)
            for col in range(2):
                at = pl.ds(col * tile, tile)
                real, imag = out[:tile, col * tile : (col + 1) * tile], out[tile:, col * tile : (col + 1) * tile]
                obj_re = patch_ref[p, 0, rows, at].astype(f32)
                obj_im = patch_ref[p, 1, rows, at].astype(f32)
                diff_re = real - exits[p, m, rows, 2 * col * tile : (2 * col + 1) * tile].astype(f32)
                diff_im = imag - exits[p, m, rows, (2 * col + 1) * tile : (2 * col + 2) * tile].astype(f32)
                add_re = obj_re * diff_re + obj_im * diff_im
                add_im = obj_re * diff_im - obj_im * diff_re
                grad[m, 0, rows, at] = jnp.where(p == 0, add_re, grad[m, 0, rows, at] + add_re)
                grad[m, 1, rows, at] = jnp.where(p == 0, add_im, grad[m, 1, rows, at] + add_im)

    def backward(p, carry):
        unfix(p)

        def one(m, carry):
            gradient(p, m)
            return carry

        lax.fori_loop(0, modes, one, 0)
        return carry

    last = positions - 1
    amp_load.wait()
    lax.fori_loop(0, last, backward, 0)
    unfix(last)
    for k in range(1, spot.count):
        pl.semaphore_signal(ready, inc=1, device_id={"grp": lax.rem(spot.me + k, spot.count)}, device_id_type=MESH)
    for copy in broadcast(spot, tile_in, tile_all, ibc_s, ibc_r):
        copy.wait()
    shift = jnp.sum(tile_all[...]) / pixels

    def held(m):
        return wave.at[0, m, 0]

    def room(m, k, slot):
        rows = scatter_sizes(shape, width)[k][1]
        at = slot * rows + tile
        if k % 2:
            return wave.at[1, m, 1, :, pl.ds(pl.multiple_of(slot * rows, 8), rows), :]
        block = at // tile
        rem = (lambda a, b: a % b) if isinstance(slot, int) else lax.rem
        return wave.at[block // 2, m, rem(block, 2), :, pl.ds(pl.multiple_of(rem(at, tile), 8), rows), :]

    def give(m):
        other = (1 - spot.core) * share.part
        return remote(
            rows_at(grad.at[m], other, share.part), held(m), core_s.at[m], core_r.at[m], spot.partner()
        )

    def scatter_parts(m, path):
        sems = [(functools.partial(room, m, k), pick(sc_s[k], m), pick(sc_r[k], m)) for k in (2 * path, 2 * path + 1)]
        return share.scatter_parts(path, functools.partial(held, m), sems)

    def gather_parts(m, path):
        sems = [(pick(ga_s[k], m), pick(ga_r[k], m)) for k in (2 * path, 2 * path + 1)]
        return share.gather_parts(path, pick(probe, m), sems)

    def home(m):
        block = rows_at(probe.at[m], share.base, share.part)
        return remote(block, block, back_s.at[m], back_r.at[m], spot.partner())

    def out(m, core, k):
        part = core * share.part
        return pltpu.make_async_copy(
            rows_at(probe.at[m], part, share.part), rows_at(pre_ref.at[m], part, share.part), out_sem.at[m, k]
        )

    told = [0, 0]

    def stream(m, path):
        give(m).wait_recv()
        add_rows(held(m), grad.at[m], share.base, share.part)
        for line, chunk, slot, send, recv in scatter_parts(m, path):
            yield from line.scatter(chunk, slot, send, recv)
        rows = pl.ds(pl.multiple_of(share.offset[path], 8), share.own)
        to = pl.ds(pl.multiple_of(share.base + share.offset[path], 8), share.own)
        light = light_own[...]
        load_prev(path, m).wait()
        g_re, g_im = held(m)[0, rows, :], held(m)[1, rows, :]
        d_re, d_im = prev[m, 0], prev[m, 1]
        den = light + shift
        p_re, p_im = g_re / den, g_im / den
        probe[m, 0, to, :] = p_re
        probe[m, 1, to, :] = p_im
        (line, chunk, send, recv), later = gather_parts(m, path)
        walk = line.gather(chunk, send, recv)
        next(walk, None)
        terms = (
            g_re * p_re + g_im * p_im,
            g_re * d_re + g_im * d_im,
            light * (p_re * p_re + p_im * p_im),
            light * (p_re * d_re + p_im * d_im),
            light * (d_re * d_re + d_im * d_im),
        )
        for k, term in enumerate(terms):
            row = 5 * m + k
            sums_in[row : row + 1, :] = jnp.sum(fold_lanes(term), axis=0, keepdims=True)
        told[path] += 1
        if told[path] == modes:
            for copy in broadcast(spot, sums_in, sums_all, bc_s, bc_r):
                copy.start()
        yield
        yield from walk
        line, chunk, send, recv = later
        yield from line.gather(chunk, send, recv)
        home(m).start()
        out(m, spot.core, 0).start()

    streams = [[stream(m, path) for m in range(modes)] for path in range(2)]
    orders = [list(turns(shape, modes, path)) for path in range(2)]

    def advance(path):
        order = orders[path]
        while order and order[0] != modes:
            next(streams[path][order.pop(0)], None)

    for m in range(modes):
        gradient(last, m)
        if m == 0:
            pl.semaphore_wait(ready, spot.count - 1)
        give(m).start()
        for path in range(2):
            orders[path].pop(0)
        per_path(spot, shape[2], advance)
    sums_all[0] = sums_in[...]

    for m in range(modes):
        home(m).wait_recv()
        out(m, 1 - spot.core, 1).start()
    for copy in broadcast(spot, sums_in, sums_all, bc_s, bc_r):
        copy.wait()
    sums_ref[...] = jnp.sum(sums_all[...], axis=0)

    def close(path):
        light_end(path)
        for m in range(modes):
            for line, chunk, slot, send, recv in scatter_parts(m, path):
                line.scatter_end(chunk, slot, send, recv)
            for line, chunk, send, recv in gather_parts(m, path):
                line.gather_end(chunk, send, recv)

    give_light().wait_send()
    for m in range(modes):
        give(m).wait_send()
        home(m).wait_send()
    per_path(spot, shape[2], close)
    for m in range(modes):
        out(m, spot.core, 0).wait()
        out(m, 1 - spot.core, 1).wait()
    for p in range(positions):
        for t in range(2):
            for k in range(1, peers):
                swap(p, t, k).wait_send()


def front(base, probe, patches, amplitude, direction):
    modes, width = probe.shape[1], probe.shape[2]
    positions = patches.shape[0]
    peers = lax.axis_size("mode")
    tile = width // 2
    dma = pltpu.SemaphoreType.DMA
    f32, bf16 = jnp.float32, jnp.bfloat16
    vmem = pl.BlockSpec(memory_space=pltpu.VMEM)
    shape = split_lines(lax.axis_size("grp"))
    outer, inner, cores = shape
    assert cores == 2 and positions >= 2
    sizes = scatter_sizes(shape, width)
    count, lanes = lax.axis_size("grp"), min(128, width)
    own = sizes[1][1]
    back_sizes = [outer, inner, inner, outer]
    sum_rows = -(-5 * modes // 8) * 8
    hbm = pl.BlockSpec(memory_space=pl.ANY)
    flops = positions * modes * 2 * 16 * width**3
    return pl.pallas_call(
        functools.partial(front_kernel, peers, shape),
        in_specs=[vmem, hbm, vmem, hbm, hbm],
        out_specs=[hbm, vmem],
        out_shape=[
            jax.ShapeDtypeStruct((modes, 2, width, width), f32),
            jax.ShapeDtypeStruct((sum_rows, lanes), f32),
        ],
        scratch_shapes=[
            pltpu.VMEM((2 * width, 2 * width), bf16),
            pltpu.VMEM((2 * width, 2 * width), bf16),
            pltpu.VMEM((modes, 2, width, width), f32),
            pltpu.VMEM((positions, modes, width, 2 * width), bf16),
            pltpu.VMEM((positions, modes, 2, 2, tile, width), f32),
            pltpu.VMEM((modes, 2 * width, width), bf16),
            pltpu.VMEM((positions, width, width), f32),
            pltpu.VMEM((max(peers - 1, 1), positions, width, width), f32),
            dma((modes,)),
            dma((max(peers - 1, 1), positions, 2)),
            dma((max(peers - 1, 1), positions, 2)),
            pltpu.VMEM((1, width, width), f32),
            pltpu.VMEM((1, width // shape[2], width), f32),
            pltpu.VMEM((8, lanes), f32),
            pltpu.VMEM((count, 8, lanes), f32),
            pltpu.VMEM((modes, 2, width, width), f32),
            pltpu.VMEM((own, width), f32),
            pltpu.VMEM((modes, 2, own, width), f32),
            pltpu.VMEM((sum_rows, lanes), f32),
            pltpu.VMEM((count, sum_rows, lanes), f32),
            *[pltpu.VMEM((n + 1, 1, rows, width), f32) for n, rows in sizes],
            *[dma((n,)) for n, _ in sizes],
            *[dma((n + 1,)) for n, _ in sizes],
            dma((1,)),
            dma((1,)),
            dma((count,)),
            dma((count,)),
            dma((modes,)),
            dma((modes,)),
            *[dma((modes, n)) for n, _ in sizes],
            *[dma((modes, n + 1)) for n, _ in sizes],
            *[dma((modes, 2, n)) for n in back_sizes],
            *[dma((modes, n)) for n in back_sizes],
            dma((modes,)),
            dma((modes,)),
            dma((modes,)),
            dma((count,)),
            dma((count,)),
            dma((modes, 2)),
            pltpu.SemaphoreType.REGULAR,
            pltpu.VMEM(amplitude.shape, amplitude.dtype),
            dma((1,)),
        ],
        compiler_params=pltpu.CompilerParams(collective_id=1, has_side_effects=True, vmem_limit_bytes=FRONT_LIMIT),
        cost_estimate=pl.CostEstimate(flops=flops, bytes_accessed=0, transcendentals=0),
        name="front",
    )(base, probe, patches, amplitude, direction)


def split_lines(count):
    cores = 2 if count % 2 == 0 else 1
    chips = count // cores
    inner = 1
    while inner * inner * 4 <= chips and chips % (inner * 2) == 0:
        inner *= 2
    return chips // inner, inner, cores


class Shares:
    def __init__(self, spot, width):
        outer, inner, cores = spot.sizes
        self.part = width // cores
        self.own = self.part // (outer * inner)
        self.base = spot.core * self.part
        self.big = (self.part // inner, self.part // outer)
        first = Line(spot, "inner", inner, spot.inner)
        second = Line(spot, "outer", outer, spot.outer)
        self.lines = ((first, second), (second, first))
        self.group = (spot.inner * self.big[0], spot.outer * self.big[1])
        self.offset = (self.group[0] + spot.outer * self.own, self.group[1] + spot.inner * self.own)

    def scatter_parts(self, path, held, sems):
        top = lambda k: rows_at(held(), k * self.big[path], self.big[path])
        low = lambda k: rows_at(held(), self.group[path] + k * self.own, self.own)
        return [(line, chunk) + pair for line, chunk, pair in zip(self.lines[path], (top, low), sems)]

    def gather_parts(self, path, whole_ref, sems):
        low = lambda k: rows_at(whole_ref(), self.base + self.group[path] + k * self.own, self.own)
        top = lambda k: rows_at(whole_ref(), self.base + k * self.big[path], self.big[path])
        return [(line, chunk) + pair for line, chunk, pair in zip(self.lines[path][::-1], (low, top), sems)]


def rows_at(ref, start, count):
    return ref.at[:, pl.ds(pl.multiple_of(start, 8), count), :]


def scatter_sizes(shape, width):
    outer, inner, cores = shape
    part = width // cores
    own = part // (outer * inner)
    return [(inner, part // inner), (outer, own), (outer, part // outer), (inner, own)]


def add_rows(into, mine, start, count):
    step = 32 if count % 32 == 0 else count

    def add(i, carry):
        rows = pl.ds(pl.multiple_of(i * step, 8), step)
        into[:, rows, :] += mine[:, pl.ds(pl.multiple_of(start + i * step, 8), step), :]
        return carry

    lax.fori_loop(0, count // step, add, 0)


def broadcast(spot, src, dst, send, recv):
    copies = []
    for step in range(1, spot.count):
        to = lax.rem(spot.me + step, spot.count)
        copies.append(remote(src, dst.at[step], send.at[step], recv.at[step], {"grp": to}))
    return copies


def per_path(spot, count, act):
    for path in range(count):
        @pl.when(spot.core == path)
        def _():
            act(path)


def turns(shape, modes, path):
    key = (*shape, modes)
    if key in ORDERS:
        return ORDERS[key][path]
    steps = 8 * (shape[0] + shape[1])
    events = sorted((k + (3 * m) // 2, m) for m in range(modes) for k in range(steps))
    return [modes] * modes + [m for _, m in events]


def finish_kernel(norm_ref, sums_ref, pre_ref, probe_ref, dir_ref, new_probe, new_dir, new_norm, kept):
    mode = pl.program_id(0)
    pixels = float(new_probe.shape[3] ** 2)

    @pl.when(pl.program_id(1) == 0)
    def _():
        index = lax.broadcasted_iota(jnp.int32, sums_ref.shape, 0)

        def mean(k):
            return jnp.sum(jnp.where(index == 5 * mode + k, sums_ref[...], 0.0)) / pixels

        norm, cross, light, light_cross, light_prev = (mean(k) for k in range(5))
        new_norm[mode] = norm
        beta = norm / norm_ref[mode]
        upper = norm + beta * cross
        lower = light + beta * (2.0 * light_cross + beta * light_prev)
        kept[0] = beta
        kept[1] = upper / (lower + 1.0)

    beta, alpha = kept[0], kept[1]
    rows = new_probe.shape[2]
    small = min(32, rows)

    def body(i, carry):
        at = pl.ds(pl.multiple_of(i * small, small), small)
        for part in range(2):
            step = pre_ref[0, part, at, :] + beta * dir_ref[part, 0, at, :]
            new_dir[part, 0, at, :] = step
            new_probe[part, 0, at, :] = probe_ref[part, 0, at, :] + alpha * step
        return carry

    lax.fori_loop(0, rows // small, body, 0)


def finish(prev_norm, sums, pre, probe, direction):
    modes, width = probe.shape[1], probe.shape[2]
    rows = min(512, width)
    block = pl.BlockSpec((2, 1, rows, width), lambda m, r: (0, m, r, 0))
    smem = pl.BlockSpec(memory_space=pltpu.SMEM)
    return pl.pallas_call(
        finish_kernel,
        grid=(modes, width // rows),
        in_specs=[
            smem,
            whole(sums.shape),
            pl.BlockSpec((1, 2, rows, width), lambda m, r: (m, 0, r, 0)),
            block,
            block,
        ],
        out_specs=[block, block, smem],
        out_shape=[
            jax.ShapeDtypeStruct(probe.shape, jnp.float32),
            jax.ShapeDtypeStruct(probe.shape, jnp.float32),
            jax.ShapeDtypeStruct((modes,), jnp.float32),
        ],
        scratch_shapes=[pltpu.SMEM((2,), jnp.float32)],
        compiler_params=pltpu.CompilerParams(
            dimension_semantics=("arbitrary", "arbitrary"), vmem_limit_bytes=FINISH_LIMIT
        ),
        name="finish",
    )(prev_norm, sums, pre, probe, direction)


def cut_kernel(offset_ref, tile_ref, patch_ref, wide):
    positions, width, full = patch_ref.shape[0], patch_ref.shape[2], tile_ref.shape[2]
    step = 64 if width % 64 == 0 else width

    def widen(i, carry):
        rows = pl.ds(pl.multiple_of(i * step, step), step)
        for part in range(2):
            wide[part, rows, :] = tile_ref[part, rows, :].astype(jnp.float32)
        return carry

    lax.fori_loop(0, full // step, widen, 0)

    def position(p, carry):
        row, col = offset_ref[p, 0], offset_ref[p, 1]
        turn = lax.rem(full - col, full)
        low = lax.rem(row, 8)
        lift = lax.rem(step + 8 - low, step + 8)

        def body(i, carry):
            for part in range(2):
                block = wide[part, pl.ds(pl.multiple_of(row - low + i * step, 8), step + 8), :]
                block = pltpu.roll(pltpu.roll(block, lift, 0)[:step], turn, 1)[:, :width]
                patch_ref[p, part, pl.ds(pl.multiple_of(i * step, step), step), :] = block.astype(jnp.bfloat16)
            return carry

        lax.fori_loop(0, width // step, body, 0)
        return carry

    lax.fori_loop(0, positions, position, 0)


def cut(offsets, tile, width):
    positions = offsets.shape[0]
    vmem = pl.BlockSpec(memory_space=pltpu.VMEM)
    return pl.pallas_call(
        cut_kernel,
        in_specs=[pl.BlockSpec(memory_space=pltpu.SMEM), vmem],
        out_specs=vmem,
        out_shape=jax.ShapeDtypeStruct((positions, 2, width, width), jnp.bfloat16),
        scratch_shapes=[pltpu.VMEM((2, tile.shape[1] + 8, tile.shape[2]), jnp.float32)],
        compiler_params=pltpu.CompilerParams(vmem_limit_bytes=CUT_LIMIT),
        cost_estimate=pl.CostEstimate(flops=10**9, bytes_accessed=0, transcendentals=0),
        name="cut",
    )(offsets, tile)


def whole(shape):
    return pl.BlockSpec(shape, lambda *_: (0,) * len(shape))


def on_device(probe, prev_direction, prev_norm, object_tile, offsets, amplitude):
    width = probe.shape[2]
    patches = cut(offsets, object_tile, width)
    pre, sums = front(base_table(width), probe, patches, amplitude, prev_direction)
    return tuple(finish(prev_norm, sums, pre, probe, prev_direction))


def solution(mesh):
    return jax.shard_map(
        on_device,
        mesh=mesh,
        in_specs=(
            P(None, "mode", None, None),
            P(None, "mode", None, None),
            P("mode"),
            P(None, "grp", None),
            P("grp", None),
            P("grp", None, None),
        ),
        out_specs=(P(None, "mode", None, None), P(None, "mode", None, None), P("mode")),
        check_vma=False,
    )
```
